256 devices in a mesh: dp: 8 (over x, core), rows: 32 (over y, z).
Axes of the slice: x: 4, y: 4, z: 8, core: 2. Of those that a mesh axis runs over, the one named last changes fastest.
Arguments:
- grads: bfloat16 [2, 4096, 14336], P(None, 'rows', 'dp'), may hold values from -64 to 64
- basis: bfloat16 [2, 4096, 512], P(None, 'rows'), may hold values from -0.09375 to 0.09375
- moment1: float32 [2, 512, 14336], P(None, 'rows', 'dp'), may hold values from -0.3 to 0.3
- moment2: float32 [2, 512, 14336], P(None, 'rows', 'dp'), may hold values from 0.001 to 0.03
- weights: bfloat16 [2, 4096, 14336], P(None, 'rows', 'dp'), may hold values from -0.09375 to 0.09375
Outputs:
- new_weights: bfloat16 [2, 4096, 14336], P(None, 'rows')
- new_moment1: float32 [2, 512, 14336], P(None, 'rows', 'dp')
- new_moment2: float32 [2, 512, 14336], P(None, 'rows', 'dp')
The draws below stay inside these ranges and needn't reach their ends.
All inputs are finite; a program needn't handle non-finite values.
Results may differ from the reference program's by a relative error of at most 0.00115.
The reference program's roundings to bfloat16 on the way count: a program that leaves them out, or rounds other values in their place, can miss the bound.
Values may be sent and summed in bfloat16 or wider, within the bound.
No kernel may reach another device: no remote copies, remote signals or barrier semaphores. Data moves between devices by JAX's collectives and lax.ppermute only.
A program may use at most 64 MiB of HBM per device.

```python
import math
import jax
import jax.numpy as jnp

D = 4096
FF = 14336
RANK = 512
MATS = 2
STEP = 10


def draw_grads(key, part):
    key_rows = jax.random.fold_in(key, 11)
    key_cols = jax.random.fold_in(key, 12)
    primary_key = jax.random.fold_in(key, 13)
    row_scale = jnp.repeat(jnp.exp(jax.random.uniform(key_rows, (MATS, D // 32, 1), jnp.float32, -0.7, 0.7)), 32, axis=1)
    col_scale = jnp.repeat(jnp.exp(jax.random.uniform(key_cols, (MATS, 1, FF // 128), jnp.float32, -0.7, 0.7)), 128, axis=2)
    values = 8.0 * jax.random.normal(primary_key, (MATS, D, FF), jnp.float32) * row_scale * col_scale
    return jnp.clip(values, -64.0, 64.0).astype(jnp.bfloat16)


def block_scale(own_key, shape, cuts, low, high):
    factor_of, own = 1.0, jax.random.fold_in(own_key, 6)
    for dim, parts in cuts:
        heights = jnp.exp(jax.random.uniform(jax.random.fold_in(own, dim), (parts,), jnp.float32, low / len(cuts), high / len(cuts)))
        factor_of = factor_of * jnp.repeat(heights, shape[dim] // parts).reshape([-1 if axis == dim else 1 for axis in range(len(shape))])
    return factor_of


def scatter_about(own_key, dims, deviation, most, cuts=(), held_as=jnp.bfloat16):
    entries = deviation * jax.random.normal(own_key, dims, jnp.float32)
    if cuts:
        entries = entries * block_scale(own_key, dims, cuts, -0.22, 0.18)
    return jnp.clip(entries, -most, most).astype(held_as)


def setup_inputs(seed: int = 0) -> dict:
    keys = jax.random.split(jax.random.key(seed), 6)
    grads = draw_grads(jax.random.fold_in(keys[5], 71), 0)
    basis = scatter_about(keys[1], (MATS, D, RANK), D ** -0.5, 0.09375, ((1, 32),))
    moment1 = scatter_about(keys[2], (MATS, RANK, FF), 0.05, 0.3, ((1, 32), (2, 8)), jnp.float32)
    moment2 = jnp.clip(jnp.exp(math.log(0.03) - 3.4011973 * jax.random.uniform(keys[3], (MATS, RANK, FF), jnp.float32) ** block_scale(keys[3], (MATS, RANK, FF), ((1, 32), (2, 8)), -0.2, 0.2)), 0.001, 0.03)
    weights = scatter_about(keys[4], (MATS, D, FF), D ** -0.5, 0.09375, ((1, 32), (2, 8)))
    return dict(grads=grads, basis=basis, moment1=moment1, moment2=moment2, weights=weights)


def reference(grads, basis, moment1, moment2, weights):
    total = jnp.float32(0.0)
    for index in range(MATS):
        grad_block = grads[index].astype(jnp.float32)
        total = total + jnp.sum(grad_block * grad_block)
    limit = 1.0 * math.sqrt(MATS * D * FF)
    scale = limit / jnp.maximum(jnp.sqrt(total), limit)
    first_bias_correction = 1.0 - 0.9 ** STEP
    second_fix = 1.0 - 0.999 ** STEP
    out_weights = []
    out_first = []
    out_second = []
    for index in range(MATS):
        base = basis[index].astype(jnp.float32)
        projected = jnp.dot(base.T, grads[index].astype(jnp.float32), preferred_element_type=jnp.float32)
        scaled = scale * projected
        first = 0.9 * moment1[index] + 0.1 * scaled
        second = 0.999 * moment2[index] + 0.001 * scaled * scaled
        low_rank_update = (first / first_bias_correction / (jnp.sqrt(second / second_fix) + 1e-08)).astype(jnp.bfloat16)
        projected_back = jnp.dot(base, low_rank_update.astype(jnp.float32), preferred_element_type=jnp.float32)
        out_weights.append((weights[index].astype(jnp.float32) - 0.5 * projected_back).astype(jnp.bfloat16))
        out_first.append(first)
        out_second.append(second)
    return (jnp.stack(out_weights), jnp.stack(out_first), jnp.stack(out_second))
```

```python
import functools
import math

import jax
import jax.numpy as jnp
from jax import lax
from jax.experimental import pallas as pl
from jax.experimental.pallas import tpu as pltpu
from jax.sharding import Mesh
from jax.sharding import PartitionSpec as P


D = 4096
FF = 14336
MATS = 2
STEP = 10
F32 = jnp.float32
BF16 = jnp.bfloat16
VMEM = pl.BlockSpec(memory_space=pltpu.VMEM)
SMEM = pl.BlockSpec(memory_space=pltpu.SMEM)
ANY = pl.BlockSpec(memory_space=pl.ANY)


def shift(v, axis, k):
    n = lax.axis_size(axis)
    return lax.ppermute(v, axis, [(i, (i + k) % n) for i in range(n)])


def exchange(v, axis):
    return lax.all_to_all(v, axis, split_axis=0, concat_axis=0, tiled=True)


def spread(v, axis):
    return exchange(jnp.broadcast_to(v[None], (lax.axis_size(axis), *v.shape)), axis)


def project_kernel(at_ref, g_ref, own_ref, peer_ref, out_ref):
    x, core = at_ref[0], at_ref[1]
    nx, nz = own_ref.shape[0], own_ref.shape[1]
    parts = out_ref.shape[0]
    width = out_ref.shape[-1]

    def run(first_ref, second_ref):
        for m in range(MATS):
            total = None
            for z in range(0, nz, 2):
                rows = []
                for zz in (z, z + 1):
                    for xa in range(nx):
                        d = lax.rem(x - xa + nx, nx)
                        rows += [first_ref[d, zz, m], second_ref[d, zz, m]]
                block = jnp.concatenate(rows, axis=0)
                left = jnp.concatenate([g_ref[z, m], g_ref[z + 1, m]], axis=1)
                term = jnp.dot(left, block, preferred_element_type=F32)
                total = term if total is None else total + term
            for y in range(parts):
                out_ref[y, m] = total[:, y * width : (y + 1) * width]

    @pl.when(core == 0)
    def _():
        run(own_ref, peer_ref)

    @pl.when(core == 1)
    def _():
        run(peer_ref, own_ref)


def project(at, g, own, peer, parts):
    nz, mats, cols, rows = g.shape
    rank = own.shape[-1]
    return pl.pallas_call(
        project_kernel,
        out_shape=jax.ShapeDtypeStruct((parts, mats, cols, rank // parts), F32),
        in_specs=[SMEM, VMEM, VMEM, VMEM],
        out_specs=VMEM,
        cost_estimate=pl.CostEstimate(
            flops=2 * nz * mats * cols * rows * rank, bytes_accessed=4 * 2**20, transcendentals=0
        ),
        name="project",
    )(at, g, own, peer)


def back_kernel(at_ref, basis_ref, w_ref, u0, u1, u2, u3, out_ref):
    y = at_ref[0]
    width = u0.shape[0]
    blocks = (u0, u1, u2, u3)
    n = len(blocks)
    total = None
    for d in range(0, n, 2):
        left = jnp.concatenate(
            [
                basis_ref[:, pl.ds(pl.multiple_of(lax.rem(y - e + n, n) * width, width), width)]
                for e in (d, d + 1)
            ],
            axis=1,
        )
        right = jnp.concatenate([blocks[d][...], blocks[d + 1][...]], axis=0)
        term = jnp.dot(left, right, preferred_element_type=F32)
        total = term if total is None else total + term
    out_ref[...] = (w_ref[...].astype(F32) - 0.5 * total).astype(BF16)


def back(at, basis, w, blocks):
    rows, cols = w.shape
    return pl.pallas_call(
        back_kernel,
        out_shape=jax.ShapeDtypeStruct((rows, cols), BF16),
        in_specs=[SMEM] + [VMEM] * 6,
        out_specs=VMEM,
        cost_estimate=pl.CostEstimate(
            flops=2 * rows * cols * basis.shape[1], bytes_accessed=3 * 2**20, transcendentals=0
        ),
        name="back",
    )(at, basis, w, *blocks)


def place_kernel(n, m, at_ref, *refs):
    blocks, out_ref, sems = refs[:n], refs[-2], refs[-1]
    width = blocks[0].shape[1]
    copies = [
        pltpu.make_async_copy(
            blocks[i],
            out_ref.at[m, :, pl.ds(pl.multiple_of(at_ref[i] * width, 128), width)],
            sems.at[i],
        )
        for i in range(n)
    ]
    for copy in copies:
        copy.start()
    for copy in copies:
        copy.wait()


def place(whole, m, at, blocks):
    n = len(blocks)
    rows, cols = blocks[0].shape
    shape = jax.ShapeDtypeStruct((MATS, rows, cols * lax.axis_size(("x", "core"))), BF16) if whole is None else whole
    given = () if whole is None else (whole,)
    return pl.pallas_call(
        functools.partial(place_kernel, n, m),
        out_shape=jax.ShapeDtypeStruct(shape.shape, BF16),
        in_specs=[SMEM] + [VMEM] * n + [ANY] * len(given),
        out_specs=ANY,
        scratch_shapes=[pltpu.SemaphoreType.DMA((n,))],
        input_output_aliases={} if whole is None else {n + 1: 0},
        cost_estimate=pl.CostEstimate(
            flops=2**20, bytes_accessed=2 * n * rows * cols * 2, transcendentals=0
        ),
        name="place",
    )(at, *blocks, *given)


def moment_step(projected, moment1, moment2, total):
    limit = 1.0 * math.sqrt(MATS * D * FF)
    scale = limit / jnp.maximum(jnp.sqrt(total), limit)
    scaled = scale * projected
    first = 0.9 * moment1 + 0.1 * scaled
    second = 0.999 * moment2 + 0.001 * scaled * scaled
    first_bias_correction = 1.0 - 0.9**STEP
    second_fix = 1.0 - 0.999**STEP
    low_rank_update = (
        first / first_bias_correction / (jnp.sqrt(second / second_fix) + 1e-08)
    ).astype(BF16)
    return (first, second, low_rank_update)


def sum_over_all(value):
    tile = jnp.full((8, 128), value, F32)
    for axis in (("x", "core"), "y", "z"):
        tile = jnp.sum(spread(tile, axis), axis=0)
    return tile[0, 0]


def local(grads, basis, moment1, moment2, weights):
    x, core = lax.axis_index("x"), lax.axis_index("core")
    y = lax.axis_index("y")
    nx, nc, ny, nz = (lax.axis_size(a) for a in ("x", "core", "y", "z"))
    mats, rows, cols = grads.shape
    rank = basis.shape[2]
    part = rows // (nx * nc)
    ranks = rank // (ny * nz)

    grad_wide = grads.astype(F32)
    total = sum_over_all(jnp.sum(grad_wide * grad_wide))

    piece = lax.dynamic_slice_in_dim(basis, (x * nc + core) * part, part, axis=1)
    held = spread(piece, "z")
    own = jnp.stack([held, shift(held, "x", 1), shift(held, "x", 2), shift(held, "x", 3)])
    peer = shift(own, "core", 1)

    turned = jnp.swapaxes(grads, 1, 2).reshape(mats, nz, cols // nz, rows)
    mine = exchange(jnp.swapaxes(turned, 0, 1), "z")
    partial = project(jnp.stack([x, core]), mine, own, peer, ny)
    summed = jnp.sum(exchange(partial, "y"), axis=0)
    by_rank = jnp.swapaxes(summed, 1, 2).reshape(mats, nz, ranks, cols // nz)
    projected = exchange(jnp.swapaxes(by_rank, 0, 1), "z")
    projected = projected.transpose(1, 2, 0, 3).reshape(mats, ranks, cols)
    first, second, update = moment_step(projected, moment1, moment2, total)

    whole = None
    at_y = jnp.stack([y])
    half = rows // 2
    for m in range(mats):
        block = spread(update[m], "z").reshape(nz * ranks, cols)
        blocks = [block] + [shift(block, "y", k) for k in (1, 2, 3)]
        fresh = back(at_y, basis[m], weights[m], blocks)
        near = [shift(fresh, "x", 1), shift(fresh, "x", -1)]
        far = jnp.concatenate(
            [shift(near[0][:half], "x", 1), shift(near[1][half:], "x", -1)], axis=0
        )
        for blocks, xs in (([fresh], [x]), (near, [x - 1, x + 1]), ([far], [x + 2])):
            ours = [lax.rem(v + nx, nx) * nc + core for v in xs]
            theirs = [lax.rem(v + nx, nx) * nc + 1 - core for v in xs]
            across = [shift(b, "core", 1) for b in blocks]
            whole = place(whole, m, jnp.stack(ours + theirs), blocks + across)
    return (whole, first, second)


def solution(mesh):
    finer = Mesh(mesh.devices.reshape(4, 2, 4, 8), ("x", "core", "y", "z"))
    dp, rows = ("x", "core"), ("y", "z")
    in_specs = (
        P(None, rows, dp),
        P(None, rows, None),
        P(None, rows, dp),
        P(None, rows, dp),
        P(None, rows, dp),
    )
    out_specs = (P(None, rows, None), P(None, rows, dp), P(None, rows, dp))
    return jax.shard_map(local, mesh=finer, in_specs=in_specs, out_specs=out_specs, check_vma=False)
```

```python
import functools
import math

import jax
import jax.numpy as jnp
from jax import lax
from jax.experimental import pallas as pl
from jax.experimental.pallas import tpu as pltpu
from jax.sharding import Mesh
from jax.sharding import PartitionSpec as P


D = 4096
FF = 14336
MATS = 2
STEP = 10
F32 = jnp.float32
BF16 = jnp.bfloat16
VMEM = pl.BlockSpec(memory_space=pltpu.VMEM)
SMEM = pl.BlockSpec(memory_space=pltpu.SMEM)
ANY = pl.BlockSpec(memory_space=pl.ANY)
PARAMS = pltpu.CompilerParams(vmem_limit_bytes=20 * 2**20)


def shift(v, axis, k):
    n = lax.axis_size(axis)
    return lax.ppermute(v, axis, [(i, (i + k) % n) for i in range(n)])


def exchange(v, axis):
    return lax.all_to_all(v, axis, split_axis=0, concat_axis=0, tiled=True)


def cost(flops, size):
    return pl.CostEstimate(flops=int(flops), bytes_accessed=int(size), transcendentals=0)


def before(first, second):
    return lax.optimization_barrier((first, second))[1]


def project_kernel(at_ref, g_ref, own_ref, peer_ref, tile_ref, *refs):
    outs, basis_ref, total_ref = refs[:-2], refs[-2], refs[-1]
    x, core, y, z = (at_ref[i] for i in range(4))
    nx, nz, _, part, _ = own_ref.shape
    cols = g_ref.shape[2]
    ny = len(outs)
    width = outs[0].shape[-1]

    def gather(zz, _):
        e = lax.rem(z - zz + nz, nz)
        for m in range(MATS):
            for xa in range(nx):
                d = lax.rem(x - xa + nx, nx)
                ours, theirs = own_ref[d, e, m], peer_ref[d, e, m]
                basis_ref[m, zz, 2 * xa * part : (2 * xa + 1) * part] = jnp.where(
                    core == 0, ours, theirs
                )
                basis_ref[m, zz, (2 * xa + 1) * part : (2 * xa + 2) * part] = jnp.where(
                    core == 0, theirs, ours
                )
        return 0

    lax.fori_loop(0, nz, gather, 0)

    def multiply(m, _):
        left = jnp.concatenate([g_ref[zz, m] for zz in range(nz)], axis=1)
        right = basis_ref[m].reshape(left.shape[1], -1)
        total_ref[m] = jnp.dot(left, right, preferred_element_type=F32)
        return 0

    lax.fori_loop(0, MATS, multiply, 0)
    for m in range(MATS):
        for d in range(ny):
            start = pl.multiple_of(lax.rem(y + d, ny) * width, width)
            outs[d][m, :cols] = total_ref[m, :, pl.ds(start, width)]
            outs[d][m, cols:] = tile_ref[...]


def project(at, g, own, peer, tile, parts):
    nz, mats, cols, rows = g.shape
    rank = own.shape[-1]
    size = (mats, cols + tile.shape[0], rank // parts)
    return pl.pallas_call(
        project_kernel,
        out_shape=[jax.ShapeDtypeStruct(size, F32)] * parts,
        in_specs=[SMEM] + [VMEM] * 4,
        out_specs=[VMEM] * parts,
        scratch_shapes=[
            pltpu.VMEM((mats, nz, rows, rank), BF16),
            pltpu.VMEM((mats, cols, rank), F32),
        ],
        compiler_params=PARAMS,
        cost_estimate=cost(2 * mats * nz * cols * rows * rank, 4 * 2**20),
        name="project",
    )(at, g, own, peer, tile)


def moments_kernel(moments_ref, p0, p1, p2, p3, new_ref, *update_refs):
    nz, _, ranks, cols = moments_ref.shape
    limit = 1.0 * math.sqrt(MATS * D * FF)
    first_bias_correction = 1.0 - 0.9**STEP
    second_fix = 1.0 - 0.999**STEP
    spare = 256 - cols
    for m in range(MATS):
        summed = (p0[m] + p1[m]) + (p2[m] + p3[m])
        scale = limit / jnp.maximum(jnp.sqrt(summed[cols : cols + 1, 0:1]), limit)
        padded = jnp.concatenate([summed[:cols], jnp.zeros((spare, summed.shape[1]), F32)], axis=0)
        scaled = scale * jnp.transpose(padded)[:, :cols]
        first = 0.9 * moments_ref[:, m].reshape(nz * ranks, cols) + 0.1 * scaled
        second = 0.999 * moments_ref[:, MATS + m].reshape(nz * ranks, cols) + 0.001 * scaled * scaled
        new_ref[:, m] = first.reshape(nz, ranks, cols)
        new_ref[:, MATS + m] = second.reshape(nz, ranks, cols)
        update = first / first_bias_correction / (jnp.sqrt(second / second_fix) + 1e-08)
        wide = jnp.concatenate([update, jnp.zeros((update.shape[0], spare), F32)], axis=1)
        turned = jnp.transpose(wide)[:cols].astype(BF16)
        for z in range(nz):
            update_refs[m][z] = turned


def moments(held, parts):
    nz, _, ranks, cols = held.shape
    return pl.pallas_call(
        moments_kernel,
        out_shape=[jax.ShapeDtypeStruct(held.shape, F32)]
        + [jax.ShapeDtypeStruct((nz, cols, nz * ranks), BF16)] * MATS,
        in_specs=[VMEM] * 5,
        out_specs=[VMEM] * (1 + MATS),
        compiler_params=PARAMS,
        cost_estimate=cost(2e9, 2 * 2**20),
        name="moments",
    )(held, *parts)


def back_kernel(m, at_ref, basis_ref, w_ref, u0, u1, u2, u3, out_ref):
    y = at_ref[2]
    width = u0.shape[1]
    blocks = (u0, u1, u2, u3)
    n = len(blocks)
    total = None
    for d in range(0, n, 2):
        left = jnp.concatenate(
            [
                basis_ref[m, :, pl.ds(pl.multiple_of(lax.rem(y - e + n, n) * width, width), width)]
                for e in (d, d + 1)
            ],
            axis=1,
        )
        right = jnp.concatenate([blocks[d][...], blocks[d + 1][...]], axis=1)
        term = lax.dot_general(
            left, right, (((1,), (1,)), ((), ())), preferred_element_type=F32
        )
        total = term if total is None else total + term
    out_ref[...] = (w_ref[m].astype(F32) - 0.5 * total).astype(BF16)


def back(m, at, basis, w, blocks):
    _, rows, cols = w.shape
    return pl.pallas_call(
        functools.partial(back_kernel, m),
        out_shape=jax.ShapeDtypeStruct((rows, cols), BF16),
        in_specs=[SMEM] + [VMEM] * 6,
        out_specs=VMEM,
        compiler_params=PARAMS,
        cost_estimate=cost(2 * rows * cols * basis.shape[2], 3 * 2**20),
        name="back",
    )(at, basis, w, *blocks)


def place_kernel(m, spots, at_ref, *refs):
    n = len(spots)
    blocks, out_ref, sems = refs[:n], refs[-2], refs[-1]
    x, core = at_ref[0], at_ref[1]
    copies = []
    for i, (dx, across, row) in enumerate(spots):
        rows, width = blocks[i].shape
        owner = lax.rem(x + dx, 4) * 2 + (1 - core if across else core)
        start = pl.multiple_of(owner * width, 128)
        copies.append(
            pltpu.make_async_copy(
                blocks[i], out_ref.at[m, pl.ds(row, rows), pl.ds(start, width)], sems.at[i]
            )
        )
    for copy in copies:
        copy.start()
    for copy in copies:
        copy.wait()


def place(whole, shape, m, at, items):
    spots = [item[1:] for item in items]
    blocks = [item[0] for item in items]
    n = len(blocks)
    given = () if whole is None else (whole,)
    size = sum(2 * 2 * b.size for b in blocks)
    return pl.pallas_call(
        functools.partial(place_kernel, m, spots),
        out_shape=jax.ShapeDtypeStruct(shape, BF16),
        in_specs=[SMEM] + [VMEM] * n + [ANY] * len(given),
        out_specs=ANY,
        scratch_shapes=[pltpu.SemaphoreType.DMA((n,))],
        input_output_aliases={} if whole is None else {n + 1: 0},
        compiler_params=PARAMS,
        cost_estimate=cost(2e9, size),
        name="place",
    )(at, *blocks, *given)


def sum_over(tile, axis):
    n = lax.axis_size(axis)
    step = 1
    while step < n:
        tile = tile + lax.ppermute(tile, axis, [(i, i ^ step) for i in range(n)])
        step *= 2
    return tile


def step(grads, basis, moment1, moment2, weights):
    x, core = lax.axis_index("x"), lax.axis_index("core")
    y, z = lax.axis_index("y"), lax.axis_index("z")
    nx, nc, ny, nz = (lax.axis_size(a) for a in ("x", "core", "y", "z"))
    mats, rows, cols = grads.shape
    rank = basis.shape[2]
    part = rows // (nx * nc)
    ranks = rank // (ny * nz)
    at = jnp.stack([x, core, y, z])

    turned = jnp.swapaxes(grads, 1, 2).reshape(mats, nz, cols // nz, rows)
    mine = exchange(jnp.swapaxes(turned, 0, 1), "z")

    piece = lax.dynamic_slice_in_dim(basis, (x * nc + core) * part, part, axis=1)
    grad_wide = turned.astype(F32)
    tile = jnp.full((8, 128), jnp.sum(grad_wide * grad_wide), F32)
    tile = sum_over(sum_over(tile, "z"), "core")
    held = jnp.stack([piece] + [shift(piece, "z", k) for k in range(1, nz)])
    tile, held = lax.optimization_barrier((tile, held))
    tile = sum_over(tile, "x")
    own = jnp.stack([held] + [shift(held, "x", k) for k in range(1, nx)])
    tile, own = lax.optimization_barrier((tile, own))
    peer = shift(own, "core", 1)

    state = jnp.concatenate([moment1, moment2], axis=0).reshape(2 * mats, ranks, nz, cols // nz)
    state = exchange(before(mine, state.transpose(2, 0, 1, 3)), "z")

    parts = project(at, mine, own, peer, tile, ny)
    parts = [parts[0]] + [shift(parts[k], "y", k) for k in range(1, ny)]
    news, *updates = moments(state, parts)
    blocks = []
    for update in updates:
        block = exchange(update, "z").reshape(cols, nz * ranks)
        blocks.append([block] + [shift(block, "y", k) for k in range(1, ny)])

    news = before(blocks[-1][0], news)
    news = exchange(news, "z").transpose(1, 2, 0, 3).reshape(2, mats, ranks, cols)

    half = rows // 2
    shape = (mats, rows, cols * nx * nc)

    def put(whole, m, items):
        there = [(shift(b, "core", 1), dx, True, row) for b, dx, row in items]
        here = [(b, dx, False, row) for b, dx, row in items]
        return place(whole, shape, m, at, here + there)

    fresh = [back(m, at, basis, weights, blocks[m]) for m in range(mats)]
    near = [(shift(f, "x", 1), shift(f, "x", -1)) for f in fresh]
    whole = put(None, 0, [(fresh[0], 0, 0)])
    whole = put(whole, 0, [(near[0][0], 3, 0), (near[0][1], 1, 0)])
    for m in range(mats):
        left, right = near[m]
        if m:
            whole, left, right = lax.optimization_barrier((whole, left, right))
            whole = put(whole, m, [(fresh[m], 0, 0)])
            whole = put(whole, m, [(left, 3, 0), (right, 1, 0)])
        top, low = shift(left[:half], "x", 1), shift(right[half:], "x", -1)
        if m:
            whole, top, low = lax.optimization_barrier((whole, top, low))
        whole = put(whole, m, [(top, 2, 0), (low, 2, half)])
    return (whole, news[0], news[1])


def solution(mesh):
    finer = Mesh(mesh.devices.reshape(4, 2, 4, 8), ("x", "core", "y", "z"))
    dp, rows = ("x", "core"), ("y", "z")
    in_specs = (
        P(None, rows, dp),
        P(None, rows, None),
        P(None, rows, dp),
        P(None, rows, dp),
        P(None, rows, dp),
    )
    out_specs = (P(None, rows, None), P(None, rows, dp), P(None, rows, dp))
    return jax.shard_map(step, mesh=finer, in_specs=in_specs, out_specs=out_specs, check_vma=False)
```

```python
import functools
import math

import jax
import jax.numpy as jnp
from jax import lax
from jax.experimental import pallas as pl
from jax.experimental.pallas import tpu as pltpu
from jax.sharding import Mesh
from jax.sharding import PartitionSpec as P


D = 4096
FF = 14336
MATS = 2
STEP = 10
F32 = jnp.float32
BF16 = jnp.bfloat16
VMEM = pl.BlockSpec(memory_space=pltpu.VMEM)
SMEM = pl.BlockSpec(memory_space=pltpu.SMEM)
ANY = pl.BlockSpec(memory_space=pl.ANY)
PARAMS = pltpu.CompilerParams(vmem_limit_bytes=20 * 2**20)


def shift(v, axis, k):
    n = lax.axis_size(axis)
    return lax.ppermute(v, axis, [(i, (i + k) % n) for i in range(n)])


def exchange(v, axis):
    return lax.all_to_all(v, axis, split_axis=0, concat_axis=0, tiled=True)


def cost(flops, size):
    return pl.CostEstimate(flops=int(flops), bytes_accessed=int(size), transcendentals=0)


def before(first, second):
    return lax.optimization_barrier((first, second))[1]


def project_kernel(at_ref, g_ref, own_ref, peer_ref, basis_ref, *refs):
    outs, total_ref = refs[:-1], refs[-1]
    x, core, y, z = (at_ref[i] for i in range(4))
    nx, nz, _, part, _ = own_ref.shape
    ny = len(outs)
    width = outs[0].shape[-1]

    def gather(zz, _):
        e = lax.rem(z - zz + nz, nz)
        for m in range(MATS):
            for xa in range(nx):
                d = lax.rem(x - xa + nx, nx)
                ours, theirs = own_ref[d, e, m], peer_ref[d, e, m]
                basis_ref[m, zz, 2 * xa * part : (2 * xa + 1) * part] = jnp.where(
                    core == 0, ours, theirs
                )
                basis_ref[m, zz, (2 * xa + 1) * part : (2 * xa + 2) * part] = jnp.where(
                    core == 0, theirs, ours
                )
        return 0

    lax.fori_loop(0, nz, gather, 0)

    def multiply(m, _):
        left = jnp.concatenate([g_ref[zz, m] for zz in range(nz)], axis=1)
        right = basis_ref[m].reshape(left.shape[1], -1)
        total_ref[m] = jnp.dot(left, right, preferred_element_type=F32)
        return 0

    lax.fori_loop(0, MATS, multiply, 0)
    for d in range(ny):
        start = pl.multiple_of(lax.rem(y + d, ny) * width, width)
        outs[d][...] = total_ref[:, :, pl.ds(start, width)]


def project(at, g, own, peer, parts):
    nz, mats, cols, rows = g.shape
    rank = own.shape[-1]
    basis, *out = pl.pallas_call(
        project_kernel,
        out_shape=[jax.ShapeDtypeStruct((mats, nz, rows, rank), BF16)]
        + [jax.ShapeDtypeStruct((mats, cols, rank // parts), F32)] * parts,
        in_specs=[SMEM] + [VMEM] * 3,
        out_specs=[VMEM] * (1 + parts),
        scratch_shapes=[pltpu.VMEM((mats, cols, rank), F32)],
        compiler_params=PARAMS,
        cost_estimate=cost(2 * mats * nz * cols * rows * rank, 4 * 2**20),
        name="project",
    )(at, g, own, peer)
    return basis, out


def moments_kernel(moments_ref, sum_ref, new_ref, update_ref):
    nz, _, cols = moments_ref.shape
    kinds = 2 * MATS
    ranks = new_ref.shape[1] // kinds
    limit = 1.0 * math.sqrt(MATS * D * FF)
    total = jnp.sum(moments_ref[:, kinds * ranks :], axis=0)
    scale = limit / jnp.maximum(jnp.sqrt(total[0:1, 0:1]), limit)
    first_bias_correction = 1.0 - 0.9**STEP
    second_fix = 1.0 - 0.999**STEP
    spare = 256 - cols
    for m in range(MATS):
        one, two = (slice(k * ranks, (k + 1) * ranks) for k in (m, MATS + m))
        summed = sum_ref[m]
        padded = jnp.concatenate([summed, jnp.zeros((spare, summed.shape[1]), F32)], axis=0)
        scaled = scale * jnp.transpose(padded)[:, :cols]
        first = 0.9 * moments_ref[:, one].reshape(nz * ranks, cols) + 0.1 * scaled
        second = 0.999 * moments_ref[:, two].reshape(nz * ranks, cols) + 0.001 * scaled * scaled
        new_ref[:, one] = first.reshape(nz, ranks, cols)
        new_ref[:, two] = second.reshape(nz, ranks, cols)
        update = first / first_bias_correction / (jnp.sqrt(second / second_fix) + 1e-08)
        wide = jnp.concatenate([update, jnp.zeros((update.shape[0], spare), F32)], axis=1)
        update_ref[m] = jnp.transpose(wide)[:cols].astype(BF16)


def moments(held, ranks, summed):
    nz, _, cols = held.shape
    return pl.pallas_call(
        moments_kernel,
        out_shape=[
            jax.ShapeDtypeStruct((nz, 2 * MATS * ranks, cols), F32),
            jax.ShapeDtypeStruct((MATS, cols, nz * ranks), BF16),
        ],
        in_specs=[VMEM] * 2,
        out_specs=[VMEM] * 2,
        compiler_params=PARAMS,
        cost_estimate=cost(2e9, 2 * 2**20),
        name="moments",
    )(held, summed)


def back_kernel(m, at_ref, basis_ref, w_ref, u0, u1, u2, u3, out_ref, whole_ref):
    y = at_ref[2]
    width = u0.shape[2]
    blocks = (u0, u1, u2, u3)
    n = len(blocks)
    for d in range(n):
        start = pl.multiple_of(lax.rem(y - d + n, n) * width, width)
        whole_ref[:, pl.ds(start, width)] = blocks[d][m]

    def rows(z, _):
        product = lax.dot_general(
            whole_ref[...], basis_ref[m, z], (((1,), (1,)), ((), ())), preferred_element_type=F32
        )
        out_ref[z] = (w_ref[z, m].astype(F32) - 0.5 * product).astype(BF16)
        return 0

    lax.fori_loop(0, basis_ref.shape[1], rows, 0)


def back(m, at, basis, w, blocks):
    nz, _, cols, rows = w.shape
    rank = basis.shape[3]
    return pl.pallas_call(
        functools.partial(back_kernel, m),
        out_shape=jax.ShapeDtypeStruct((nz, cols, rows), BF16),
        in_specs=[SMEM] + [VMEM] * 6,
        out_specs=VMEM,
        scratch_shapes=[pltpu.VMEM((cols, rank), BF16)],
        compiler_params=PARAMS,
        cost_estimate=cost(2 * nz * rows * cols * rank, 3 * 2**20),
        name="back",
    )(at, basis, w, *blocks)


def place_kernel(m, spots, at_ref, *refs):
    n = len(spots)
    blocks, out_ref, sems = refs[:n], refs[-2], refs[-1]
    x, core = at_ref[0], at_ref[1]
    copies = []
    for i, (dx, across, row) in enumerate(spots):
        rows, width = blocks[i].shape
        owner = lax.rem(x + dx, 4) * 2 + (1 - core if across else core)
        start = pl.multiple_of(owner * width, 128)
        copies.append(
            pltpu.make_async_copy(
                blocks[i], out_ref.at[m, pl.ds(row, rows), pl.ds(start, width)], sems.at[i]
            )
        )
    for copy in copies:
        copy.start()
    for copy in copies:
        copy.wait()


def place(whole, shape, m, at, items):
    spots = [item[1:] for item in items]
    blocks = [item[0] for item in items]
    n = len(blocks)
    given = () if whole is None else (whole,)
    size = sum(2 * 2 * b.size for b in blocks)
    return pl.pallas_call(
        functools.partial(place_kernel, m, spots),
        out_shape=jax.ShapeDtypeStruct(shape, BF16),
        in_specs=[SMEM] + [VMEM] * n + [ANY] * len(given),
        out_specs=ANY,
        scratch_shapes=[pltpu.SemaphoreType.DMA((n,))],
        input_output_aliases={} if whole is None else {n + 1: 0},
        compiler_params=PARAMS,
        cost_estimate=cost(2e9, size),
        name="place",
    )(at, *blocks, *given)


def sum_over(tile, axis):
    n = lax.axis_size(axis)
    step = 1
    while step < n:
        tile = tile + lax.ppermute(tile, axis, [(i, i ^ step) for i in range(n)])
        step *= 2
    return tile


def step(grads, basis, moment1, moment2, weights):
    x, core = lax.axis_index("x"), lax.axis_index("core")
    y, z = lax.axis_index("y"), lax.axis_index("z")
    nx, nc, ny, nz = (lax.axis_size(a) for a in ("x", "core", "y", "z"))
    mats, rows, cols = grads.shape
    rank = basis.shape[2]
    part = rows // (nx * nc)
    ranks = rank // (ny * nz)
    at = jnp.stack([x, core, y, z])

    def by_block(v):
        blocks = jnp.swapaxes(v, 1, 2).reshape(mats, nz, cols // nz, rows)
        return blocks, jnp.swapaxes(blocks, 0, 1)

    piece = lax.dynamic_slice_in_dim(basis, (x * nc + core) * part, part, axis=1)
    held = jnp.stack([piece] + [shift(piece, "z", k) for k in range(1, nz)])
    turned, sent = by_block(grads)
    mine = exchange(sent, "z")
    grad_wide = turned.astype(F32)
    tile = jnp.full((8, cols // nz), jnp.sum(grad_wide * grad_wide), F32)
    tile = sum_over(tile, "x")
    tile, held = lax.optimization_barrier((tile, held))
    tile = sum_over(tile, "y")
    own = jnp.stack([held] + [shift(held, "x", k) for k in range(1, nx)])
    tile, own = lax.optimization_barrier((tile, own))
    tile = sum_over(tile, "core")
    peer = shift(own, "core", 1)

    state = jnp.concatenate([moment1, moment2], axis=0).reshape(2 * mats * ranks, nz, cols // nz)
    state = jnp.concatenate([jnp.swapaxes(state, 0, 1), jnp.stack([tile] * nz)], axis=1)
    w = by_block(weights)[1]
    mine, peer, state, w = lax.optimization_barrier((mine, peer, state, w))
    state = exchange(state, "z")

    gathered, parts = project(at, mine, own, peer, ny)
    gathered, w = lax.optimization_barrier((gathered, w))
    w = exchange(before(state, w), "z")
    parts = [parts[0]] + [shift(parts[k], "y", k) for k in range(1, ny)]
    summed = (parts[0] + parts[1]) + (parts[2] + parts[3])
    news, update = moments(state, ranks, summed)
    updates = [update] + [shift(update, "y", k) for k in range(1, ny)]
    fresh = [exchange(back(m, at, gathered, w, updates), "z") for m in range(mats)]
    news = exchange(before(fresh[-1], news), "z")
    news = jnp.swapaxes(news, 0, 1).reshape(2, mats, ranks, cols)
    fresh = [jnp.swapaxes(f.reshape(cols, rows), 0, 1) for f in fresh]

    half = rows // 2
    shape = (mats, rows, cols * nx * nc)

    def put(whole, m, items):
        there = [(shift(b, "core", 1), dx, True, row) for b, dx, row in items]
        here = [(b, dx, False, row) for b, dx, row in items]
        return place(whole, shape, m, at, here + there)

    near = [(shift(f, "x", 1), shift(f, "x", -1)) for f in fresh]
    whole = put(None, 0, [(fresh[0], 0, 0)])
    whole = put(whole, 0, [(near[0][0], 3, 0), (near[0][1], 1, 0)])
    for m in range(mats):
        left, right = near[m]
        if m:
            whole, left, right = lax.optimization_barrier((whole, left, right))
            whole = put(whole, m, [(fresh[m], 0, 0)])
            whole = put(whole, m, [(left, 3, 0), (right, 1, 0)])
        top, low = shift(left[:half], "x", 1), shift(right[half:], "x", -1)
        if m:
            whole, top, low = lax.optimization_barrier((whole, top, low))
        whole = put(whole, m, [(top, 2, 0), (low, 2, half)])
    return (whole, news[0], news[1])


def solution(mesh):
    finer = Mesh(mesh.devices.reshape(4, 2, 4, 8), ("x", "core", "y", "z"))
    dp, rows = ("x", "core"), ("y", "z")
    in_specs = (
        P(None, rows, dp),
        P(None, rows, None),
        P(None, rows, dp),
        P(None, rows, dp),
        P(None, rows, dp),
    )
    out_specs = (P(None, rows, None), P(None, rows, dp), P(None, rows, dp))
    return jax.shard_map(step, mesh=finer, in_specs=in_specs, out_specs=out_specs, check_vma=False)
```

```python
import functools
import math

import jax
import jax.numpy as jnp
from jax import lax
from jax.experimental import pallas as pl
from jax.experimental.pallas import tpu as pltpu
from jax.sharding import Mesh
from jax.sharding import PartitionSpec as P


D = 4096
FF = 14336
MATS = 2
STEP = 10
F32 = jnp.float32
BF16 = jnp.bfloat16
VMEM = pl.BlockSpec(memory_space=pltpu.VMEM)
SMEM = pl.BlockSpec(memory_space=pltpu.SMEM)
ANY = pl.BlockSpec(memory_space=pl.ANY)
PARAMS = pltpu.CompilerParams(vmem_limit_bytes=20 * 2**20)


def shift(v, axis, k):
    n = lax.axis_size(axis)
    return lax.ppermute(v, axis, [(i, (i + k) % n) for i in range(n)])


def exchange(v, axis):
    return lax.all_to_all(v, axis, split_axis=0, concat_axis=0, tiled=True)


def cost(flops, size):
    return pl.CostEstimate(flops=int(flops), bytes_accessed=int(size), transcendentals=0)


def before(first, second):
    return lax.optimization_barrier((first, second))[1]


def pack_kernel(extra, at_ref, v_ref, *refs):
    out_ref = refs[-2] if extra else refs[-1]
    nz = out_ref.shape[0]
    cols = v_ref.shape[2] // nz
    total = None
    for m in range(MATS):
        turned = jnp.transpose(v_ref[m])
        for z in range(nz):
            out_ref[z, m, :cols] = turned[z * cols : (z + 1) * cols]
        if extra:
            wide = v_ref[m].astype(F32)
            squares = jnp.sum(wide * wide, axis=0, keepdims=True)
            total = squares if total is None else total + squares
    if extra:
        basis_ref, tile_ref = refs[0], refs[-1]
        tile_ref[...] = jnp.broadcast_to(jnp.sum(total, axis=1, keepdims=True), tile_ref.shape)
        part = basis_ref.shape[1] // 8
        start = pl.multiple_of((at_ref[0] * 2 + at_ref[1]) * part, part)
        width = out_ref.shape[3]
        for m in range(MATS):
            piece = basis_ref[m, pl.ds(start, part)]
            for k in range(piece.shape[1] // width):
                low = cols + k * part
                for z in range(nz):
                    out_ref[z, m, low : low + part] = piece[:, k * width : (k + 1) * width]


def pack(at, v, nz, basis=None):
    mats, rows, cols = v.shape
    cols //= nz
    extra = basis is not None
    more = basis.shape[1] // 8 * (basis.shape[2] // rows) if extra else 0
    shapes = [jax.ShapeDtypeStruct((nz, mats, cols + more, rows), BF16)]
    if extra:
        shapes.append(jax.ShapeDtypeStruct((8, cols), F32))
    given = (basis,) if extra else ()
    out = pl.pallas_call(
        functools.partial(pack_kernel, extra),
        out_shape=shapes,
        in_specs=[SMEM] + [VMEM] * (1 + len(given)),
        out_specs=[VMEM] * len(shapes),
        compiler_params=PARAMS,
        cost_estimate=cost(2e9, 2 * 2**20),
        name="pack",
    )(at, v, *given)
    return out if extra else out[0]


def pack_state_kernel(one_ref, two_ref, tile_ref, out_ref):
    nz, _, cols = out_ref.shape
    ranks = one_ref.shape[1]
    for k, ref in enumerate((one_ref, two_ref)):
        for m in range(MATS):
            low = (k * MATS + m) * ranks
            for z in range(nz):
                out_ref[z, low : low + ranks] = ref[m, :, z * cols : (z + 1) * cols]
    for z in range(nz):
        out_ref[z, 2 * MATS * ranks :] = tile_ref[...]


def pack_state(one, two, tile, nz):
    mats, ranks, cols = one.shape
    return pl.pallas_call(
        pack_state_kernel,
        out_shape=jax.ShapeDtypeStruct((nz, 2 * mats * ranks + tile.shape[0], cols // nz), F32),
        in_specs=[VMEM] * 3,
        out_specs=VMEM,
        compiler_params=PARAMS,
        cost_estimate=cost(2e9, 2**20),
        name="pack_state",
    )(one, two, tile)


def unpack_state_kernel(in_ref, one_ref, two_ref):
    nz, _, _ = in_ref.shape
    ranks = one_ref.shape[1]
    for k, ref in enumerate((one_ref, two_ref)):
        for m in range(MATS):
            low = (k * MATS + m) * ranks
            ref[m] = jnp.concatenate([in_ref[z, low : low + ranks] for z in range(nz)], axis=1)


def unpack_state(held):
    nz, kinds, cols = held.shape
    shape = jax.ShapeDtypeStruct((MATS, kinds // (2 * MATS), nz * cols), F32)
    return pl.pallas_call(
        unpack_state_kernel,
        out_shape=[shape, shape],
        in_specs=[VMEM],
        out_specs=[VMEM] * 2,
        compiler_params=PARAMS,
        cost_estimate=cost(2e9, 2**20),
        name="unpack_state",
    )(held)


def project_kernel(at_ref, g_ref, own_ref, peer_ref, basis_ref, *refs):
    outs, total_ref = refs[:-1], refs[-1]
    x, core, y = (at_ref[i] for i in range(3))
    nx, nz, _, size, width = own_ref.shape
    rank = basis_ref.shape[3]
    part = size * width // rank
    cols = total_ref.shape[1]
    ny = len(outs)

    def gather(z, _):
        for m in range(MATS):
            for xa in range(nx):
                d = lax.rem(x - xa + nx, nx)
                ours, theirs = own_ref[d, z, m], peer_ref[d, z, m]
                pair = (jnp.where(core == 0, ours, theirs), jnp.where(core == 0, theirs, ours))
                for c in range(2):
                    low = (2 * xa + c) * part
                    for k in range(rank // width):
                        basis_ref[m, z, low : low + part, k * width : (k + 1) * width] = pair[c][
                            k * part : (k + 1) * part
                        ]
        return 0

    lax.fori_loop(0, nz, gather, 0)

    def multiply(m, _):
        left = jnp.concatenate([g_ref[z, m, :cols] for z in range(nz)], axis=1)
        right = basis_ref[m].reshape(left.shape[1], -1)
        total_ref[m] = jnp.dot(left, right, preferred_element_type=F32)
        return 0

    lax.fori_loop(0, MATS, multiply, 0)
    for d in range(ny):
        start = pl.multiple_of(lax.rem(y + d, ny) * width, width)
        outs[d][...] = total_ref[:, :, pl.ds(start, width)]


def project(at, g, own, peer, cols, rank, parts):
    nz, mats, _, rows = g.shape
    basis, *out = pl.pallas_call(
        project_kernel,
        out_shape=[jax.ShapeDtypeStruct((mats, nz, rows, rank), BF16)]
        + [jax.ShapeDtypeStruct((mats, cols, rank // parts), F32)] * parts,
        in_specs=[SMEM] + [VMEM] * 3,
        out_specs=[VMEM] * (1 + parts),
        scratch_shapes=[pltpu.VMEM((mats, cols, rank), F32)],
        compiler_params=PARAMS,
        cost_estimate=cost(2 * mats * nz * cols * rows * rank, 4 * 2**20),
        name="project",
    )(at, g, own, peer)
    return basis, out


def moments_kernel(moments_ref, sum_ref, new_ref, update_ref):
    nz, _, cols = moments_ref.shape
    kinds = 2 * MATS
    ranks = new_ref.shape[1] // kinds
    limit = 1.0 * math.sqrt(MATS * D * FF)
    total = jnp.sum(moments_ref[:, kinds * ranks :], axis=0)
    scale = limit / jnp.maximum(jnp.sqrt(total[0:1, 0:1]), limit)
    first_bias_correction = 1.0 - 0.9**STEP
    second_fix = 1.0 - 0.999**STEP
    spare = 256 - cols
    for m in range(MATS):
        one, two = (slice(k * ranks, (k + 1) * ranks) for k in (m, MATS + m))
        summed = sum_ref[m]
        padded = jnp.concatenate([summed, jnp.zeros((spare, summed.shape[1]), F32)], axis=0)
        scaled = scale * jnp.transpose(padded)[:, :cols]
        first = 0.9 * moments_ref[:, one].reshape(nz * ranks, cols) + 0.1 * scaled
        second = 0.999 * moments_ref[:, two].reshape(nz * ranks, cols) + 0.001 * scaled * scaled
        new_ref[:, one] = first.reshape(nz, ranks, cols)
        new_ref[:, two] = second.reshape(nz, ranks, cols)
        update = first / first_bias_correction / (jnp.sqrt(second / second_fix) + 1e-08)
        wide = jnp.concatenate([update, jnp.zeros((update.shape[0], spare), F32)], axis=1)
        update_ref[m] = jnp.transpose(wide)[:cols].astype(BF16)


def moments(held, ranks, summed):
    nz, _, cols = held.shape
    return pl.pallas_call(
        moments_kernel,
        out_shape=[
            jax.ShapeDtypeStruct((nz, 2 * MATS * ranks, cols), F32),
            jax.ShapeDtypeStruct((MATS, cols, nz * ranks), BF16),
        ],
        in_specs=[VMEM] * 2,
        out_specs=[VMEM] * 2,
        compiler_params=PARAMS,
        cost_estimate=cost(2e9, 2 * 2**20),
        name="moments",
    )(held, summed)


def back_kernel(m, at_ref, basis_ref, w_ref, u0, u1, u2, u3, out_ref, whole_ref):
    y = at_ref[2]
    width = u0.shape[2]
    blocks = (u0, u1, u2, u3)
    n = len(blocks)
    for d in range(n):
        start = pl.multiple_of(lax.rem(y - d + n, n) * width, width)
        whole_ref[:, pl.ds(start, width)] = blocks[d][m]

    def rows(z, _):
        product = lax.dot_general(
            whole_ref[...], basis_ref[m, z], (((1,), (1,)), ((), ())), preferred_element_type=F32
        )
        out_ref[z] = (w_ref[z, m].astype(F32) - 0.5 * product).astype(BF16)
        return 0

    lax.fori_loop(0, basis_ref.shape[1], rows, 0)


def back(m, at, basis, w, blocks):
    nz, _, cols, rows = w.shape
    rank = basis.shape[3]
    return pl.pallas_call(
        functools.partial(back_kernel, m),
        out_shape=jax.ShapeDtypeStruct((nz, cols, rows), BF16),
        in_specs=[SMEM] + [VMEM] * 6,
        out_specs=VMEM,
        scratch_shapes=[pltpu.VMEM((cols, rank), BF16)],
        compiler_params=PARAMS,
        cost_estimate=cost(2 * nz * rows * cols * rank, 3 * 2**20),
        name="back",
    )(at, basis, w, *blocks)


def place_kernel(m, spots, at_ref, *refs):
    n = len(spots)
    blocks, out_ref, sems = refs[:n], refs[-2], refs[-1]
    x, core = at_ref[0], at_ref[1]
    copies = []
    for i, (dx, across, row) in enumerate(spots):
        rows, width = blocks[i].shape
        owner = lax.rem(x + dx, 4) * 2 + (1 - core if across else core)
        start = pl.multiple_of(owner * width, 128)
        copies.append(
            pltpu.make_async_copy(
                blocks[i], out_ref.at[m, pl.ds(row, rows), pl.ds(start, width)], sems.at[i]
            )
        )
    for copy in copies:
        copy.start()
    for copy in copies:
        copy.wait()


def place(whole, shape, m, at, items):
    spots = [item[1:] for item in items]
    blocks = [item[0] for item in items]
    n = len(blocks)
    given = () if whole is None else (whole,)
    size = sum(2 * 2 * b.size for b in blocks)
    return pl.pallas_call(
        functools.partial(place_kernel, m, spots),
        out_shape=jax.ShapeDtypeStruct(shape, BF16),
        in_specs=[SMEM] + [VMEM] * n + [ANY] * len(given),
        out_specs=ANY,
        scratch_shapes=[pltpu.SemaphoreType.DMA((n,))],
        input_output_aliases={} if whole is None else {n + 1: 0},
        compiler_params=PARAMS,
        cost_estimate=cost(2e9, size),
        name="place",
    )(at, *blocks, *given)


def sum_over(tile, axis):
    n = lax.axis_size(axis)
    step = 1
    while step < n:
        tile = tile + lax.ppermute(tile, axis, [(i, i ^ step) for i in range(n)])
        step *= 2
    return tile


def step(grads, basis, moment1, moment2, weights):
    x, core = lax.axis_index("x"), lax.axis_index("core")
    y, z = lax.axis_index("y"), lax.axis_index("z")
    nx, nc, ny, nz = (lax.axis_size(a) for a in ("x", "core", "y", "z"))
    mats, rows, cols = grads.shape
    rank = basis.shape[2]
    ranks = rank // (ny * nz)
    at = jnp.stack([x, core, y, z])

    sent, tile = pack(at, grads, nz, basis)
    mine = exchange(sent, "z")
    for axis in ("x", "y", "core"):
        tile = sum_over(tile, axis)
    state = pack_state(moment1, moment2, tile, nz)
    w = pack(at, weights, nz)

    held = mine[:, :, cols // nz :]
    own = jnp.stack([held] + [shift(held, "x", k) for k in range(1, nx)])
    peer = shift(own, "core", 1)
    state = exchange(before(mine, state), "z")
    w = exchange(before(state, w), "z")

    gathered, parts = project(at, mine, own, peer, cols // nz, rank, ny)
    parts = [parts[0]] + [shift(parts[k], "y", k) for k in range(1, ny)]
    summed = (parts[0] + parts[1]) + (parts[2] + parts[3])
    news, update = moments(state, ranks, summed)
    updates = [update] + [shift(update, "y", k) for k in range(1, ny)]
    fresh = [exchange(back(m, at, gathered, w, updates), "z") for m in range(mats)]
    news = unpack_state(exchange(before(fresh[-1], news), "z"))
    fresh = [jnp.swapaxes(f.reshape(cols, rows), 0, 1) for f in fresh]

    half = rows // 2
    shape = (mats, rows, cols * nx * nc)

    def put(whole, m, items):
        there = [(shift(b, "core", 1), dx, True, row) for b, dx, row in items]
        here = [(b, dx, False, row) for b, dx, row in items]
        return place(whole, shape, m, at, here + there)

    near = [(shift(f, "x", 1), shift(f, "x", -1)) for f in fresh]
    whole = put(None, 0, [(fresh[0], 0, 0)])
    whole = put(whole, 0, [(near[0][0], 3, 0), (near[0][1], 1, 0)])
    for m in range(mats):
        left, right = near[m]
        if m:
            whole, left, right = lax.optimization_barrier((whole, left, right))
            whole = put(whole, m, [(fresh[m], 0, 0)])
            whole = put(whole, m, [(left, 3, 0), (right, 1, 0)])
        top, low = shift(left[:half], "x", 1), shift(right[half:], "x", -1)
        if m:
            whole, top, low = lax.optimization_barrier((whole, top, low))
        whole = put(whole, m, [(top, 2, 0), (low, 2, half)])
    return (whole, news[0], news[1])


def solution(mesh):
    finer = Mesh(mesh.devices.reshape(4, 2, 4, 8), ("x", "core", "y", "z"))
    dp, rows = ("x", "core"), ("y", "z")
    in_specs = (
        P(None, rows, dp),
        P(None, rows, None),
        P(None, rows, dp),
        P(None, rows, dp),
        P(None, rows, dp),
    )
    out_specs = (P(None, rows, None), P(None, rows, dp), P(None, rows, dp))
    return jax.shard_map(step, mesh=finer, in_specs=in_specs, out_specs=out_specs, check_vma=False)
```

```python
import functools
import math

import jax
import jax.numpy as jnp
from jax import lax
from jax.experimental import pallas as pl
from jax.experimental.pallas import tpu as pltpu
from jax.sharding import Mesh
from jax.sharding import PartitionSpec as P


D = 4096
FF = 14336
MATS = 2
STEP = 10
F32 = jnp.float32
BF16 = jnp.bfloat16
VMEM = pl.BlockSpec(memory_space=pltpu.VMEM)
SMEM = pl.BlockSpec(memory_space=pltpu.SMEM)
ANY = pl.BlockSpec(memory_space=pl.ANY)
PARAMS = pltpu.CompilerParams(vmem_limit_bytes=20 * 2**20)


def shift(v, axis, k):
    n = lax.axis_size(axis)
    return lax.ppermute(v, axis, [(i, (i + k) % n) for i in range(n)])


def exchange(v, axis):
    return lax.all_to_all(v, axis, split_axis=0, concat_axis=0, tiled=True)


def cost(flops, size):
    return pl.CostEstimate(flops=int(flops), bytes_accessed=int(size), transcendentals=0)


def before(first, second):
    return lax.optimization_barrier((first, second))[1]


def pack_kernel(v_ref, out_ref):
    nz, _, cols, _ = out_ref.shape
    for m in range(MATS):
        turned = jnp.transpose(v_ref[m])
        for z in range(nz):
            out_ref[z, m] = turned[z * cols : (z + 1) * cols]


def pack(v, nz):
    mats, rows, cols = v.shape
    return pl.pallas_call(
        pack_kernel,
        out_shape=jax.ShapeDtypeStruct((nz, mats, cols // nz, rows), BF16),
        in_specs=[VMEM],
        out_specs=VMEM,
        compiler_params=PARAMS,
        cost_estimate=cost(2e9, 2 * 2**20),
        name="pack",
    )(v)


def pieces_kernel(at_ref, v_ref, basis_ref, out_ref):
    nz, size, width = out_ref.shape
    part = basis_ref.shape[1] // 8
    start = pl.multiple_of((at_ref[0] * 2 + at_ref[1]) * part, part)
    total = None
    for m in range(MATS):
        wide = v_ref[m].astype(F32)
        squares = jnp.sum(wide * wide, axis=0, keepdims=True)
        total = squares if total is None else total + squares
        piece = basis_ref[m, pl.ds(start, part)]
        count = piece.shape[1] // width
        for k in range(count):
            low = (m * count + k) * part
            for z in range(nz):
                out_ref[z, low : low + part] = piece[:, k * width : (k + 1) * width]
    total = jnp.sum(total, axis=1, keepdims=True)
    high = total.astype(BF16).astype(F32)
    middle = (total - high).astype(BF16).astype(F32)
    low = total - high - middle
    row = lax.broadcasted_iota(jnp.int32, (part, width), 0)
    tile = jnp.where(row == 0, high, jnp.where(row == 1, middle, jnp.where(row == 2, low, 0.0)))
    for z in range(nz):
        out_ref[z, size - part :] = tile.astype(BF16)


def pieces(at, v, basis, nz):
    mats, rows, rank = basis.shape
    part, width = rows // 8, 128
    return pl.pallas_call(
        pieces_kernel,
        out_shape=jax.ShapeDtypeStruct((nz, mats * part * rank // width + part, width), BF16),
        in_specs=[SMEM, VMEM, VMEM],
        out_specs=VMEM,
        compiler_params=PARAMS,
        cost_estimate=cost(2e9, 2**20),
        name="pieces",
    )(at, v, basis)


def pack_state_kernel(at_ref, one_ref, two_ref, *refs):
    outs, held_ref = refs[:-1], refs[-1]
    nz, _, cols = held_ref.shape
    ranks = one_ref.shape[1]
    for k, ref in enumerate((one_ref, two_ref)):
        for m in range(MATS):
            low = (k * MATS + m) * ranks
            for z in range(nz):
                held_ref[z, low : low + ranks] = ref[m, :, z * cols : (z + 1) * cols]
    for d in range(nz):
        outs[d][...] = held_ref[lax.rem(at_ref[3] + d, nz)]


def pack_state(at, one, two, nz):
    mats, ranks, cols = one.shape
    size = (2 * mats * ranks, cols // nz)
    return pl.pallas_call(
        pack_state_kernel,
        out_shape=[jax.ShapeDtypeStruct(size, F32)] * nz,
        in_specs=[SMEM, VMEM, VMEM],
        out_specs=[VMEM] * nz,
        scratch_shapes=[pltpu.VMEM((nz, *size), F32)],
        compiler_params=PARAMS,
        cost_estimate=cost(2e9, 2**20),
        name="pack_state",
    )(at, one, two)


def unpack_state_kernel(in_ref, one_ref, two_ref):
    nz, _, _ = in_ref.shape
    ranks = one_ref.shape[1]
    for k, ref in enumerate((one_ref, two_ref)):
        for m in range(MATS):
            low = (k * MATS + m) * ranks
            ref[m] = jnp.concatenate([in_ref[z, low : low + ranks] for z in range(nz)], axis=1)


def unpack_state(held):
    nz, kinds, cols = held.shape
    shape = jax.ShapeDtypeStruct((MATS, kinds // (2 * MATS), nz * cols), F32)
    return pl.pallas_call(
        unpack_state_kernel,
        out_shape=[shape, shape],
        in_specs=[VMEM],
        out_specs=[VMEM] * 2,
        compiler_params=PARAMS,
        cost_estimate=cost(2e9, 2**20),
        name="unpack_state",
    )(held)


def project_kernel(at_ref, g_ref, own_ref, peer_ref, basis_ref, *refs):
    outs, total_ref = refs[:-1], refs[-1]
    x, core, y = (at_ref[i] for i in range(3))
    nx, nz, size, width = own_ref.shape
    rank = basis_ref.shape[3]
    part = basis_ref.shape[2] // (2 * nx)
    count = rank // width
    cols = g_ref.shape[2]
    ny = len(outs)

    def gather(z, _):
        for m in range(MATS):
            for xa in range(nx):
                d = lax.rem(x - xa + nx, nx)
                for k in range(count):
                    low = (m * count + k) * part
                    ours, theirs = own_ref[d, z, low : low + part], peer_ref[d, z, low : low + part]
                    at = 2 * xa * part
                    lanes = slice(k * width, (k + 1) * width)
                    basis_ref[m, z, at : at + part, lanes] = jnp.where(core == 0, ours, theirs)
                    basis_ref[m, z, at + part : at + 2 * part, lanes] = jnp.where(
                        core == 0, theirs, ours
                    )
        return 0

    lax.fori_loop(0, nz, gather, 0)

    def multiply(m, _):
        left = jnp.concatenate([g_ref[z, m] for z in range(nz)], axis=1)
        right = basis_ref[m].reshape(left.shape[1], -1)
        total_ref[m] = jnp.dot(left, right, preferred_element_type=F32)
        return 0

    lax.fori_loop(0, MATS, multiply, 0)
    squares = jnp.zeros((part, width), F32)
    for ref in (own_ref, peer_ref):
        for d in range(nx):
            for z in range(nz):
                squares = squares + ref[d, z, size - part :].astype(F32)
    squares = jnp.sum(squares, axis=0, keepdims=True)
    for d in range(ny):
        start = pl.multiple_of(lax.rem(y + d, ny) * width, width)
        outs[d][:, :cols] = total_ref[:, :, pl.ds(start, width)]
        for m in range(MATS):
            outs[d][m, cols:] = jnp.broadcast_to(squares, (8, width))


def project(at, g, own, peer, rank, parts):
    nz, mats, cols, rows = g.shape
    basis, *out = pl.pallas_call(
        project_kernel,
        out_shape=[jax.ShapeDtypeStruct((mats, nz, rows, rank), BF16)]
        + [jax.ShapeDtypeStruct((mats, cols + 8, rank // parts), F32)] * parts,
        in_specs=[SMEM] + [VMEM] * 3,
        out_specs=[VMEM] * (1 + parts),
        scratch_shapes=[pltpu.VMEM((mats, cols, rank), F32)],
        compiler_params=PARAMS,
        cost_estimate=cost(2 * mats * nz * cols * rows * rank, 4 * 2**20),
        name="project",
    )(at, g, own, peer)
    return basis, out


def moments_kernel(at_ref, sum_ref, *refs):
    held, new_ref, update_ref, held_ref = refs[:-3], refs[-3], refs[-2], refs[-1]
    nz, kinds, cols = held_ref.shape
    ranks = kinds // (2 * MATS)
    for d in range(nz):
        held_ref[lax.rem(at_ref[3] - d + nz, nz)] = held[d][...]
    limit = 1.0 * math.sqrt(MATS * D * FF)
    scale = limit / jnp.maximum(jnp.sqrt(sum_ref[0, cols : cols + 1, 0:1]), limit)
    first_bias_correction = 1.0 - 0.9**STEP
    second_fix = 1.0 - 0.999**STEP
    spare = 256 - cols
    for m in range(MATS):
        one, two = (slice(k * ranks, (k + 1) * ranks) for k in (m, MATS + m))
        summed = sum_ref[m, :cols]
        padded = jnp.concatenate([summed, jnp.zeros((spare, summed.shape[1]), F32)], axis=0)
        scaled = scale * jnp.transpose(padded)[:, :cols]
        first = 0.9 * held_ref[:, one].reshape(nz * ranks, cols) + 0.1 * scaled
        second = 0.999 * held_ref[:, two].reshape(nz * ranks, cols) + 0.001 * scaled * scaled
        new_ref[:, one] = first.reshape(nz, ranks, cols)
        new_ref[:, two] = second.reshape(nz, ranks, cols)
        update = first / first_bias_correction / (jnp.sqrt(second / second_fix) + 1e-08)
        wide = jnp.concatenate([update, jnp.zeros((update.shape[0], spare), F32)], axis=1)
        update_ref[m] = jnp.transpose(wide)[:cols].astype(BF16)


def moments(at, summed, held):
    nz = len(held)
    kinds, cols = held[0].shape
    ranks = kinds // (2 * MATS)
    return pl.pallas_call(
        moments_kernel,
        out_shape=[
            jax.ShapeDtypeStruct((nz, kinds, cols), F32),
            jax.ShapeDtypeStruct((MATS, cols, nz * ranks), BF16),
        ],
        in_specs=[SMEM] + [VMEM] * (1 + nz),
        out_specs=[VMEM] * 2,
        scratch_shapes=[pltpu.VMEM((nz, kinds, cols), F32)],
        compiler_params=PARAMS,
        cost_estimate=cost(2e9, 2 * 2**20),
        name="moments",
    )(at, summed, *held)


def back_kernel(m, at_ref, basis_ref, w_ref, u0, u1, u2, u3, out_ref, whole_ref):
    y = at_ref[2]
    width = u0.shape[2]
    blocks = (u0, u1, u2, u3)
    n = len(blocks)
    for d in range(n):
        start = pl.multiple_of(lax.rem(y - d + n, n) * width, width)
        whole_ref[:, pl.ds(start, width)] = blocks[d][m]

    def rows(z, _):
        product = lax.dot_general(
            whole_ref[...], basis_ref[m, z], (((1,), (1,)), ((), ())), preferred_element_type=F32
        )
        out_ref[z] = (w_ref[z, m].astype(F32) - 0.5 * product).astype(BF16)
        return 0

    lax.fori_loop(0, basis_ref.shape[1], rows, 0)


def back(m, at, basis, w, blocks):
    nz, _, cols, rows = w.shape
    rank = basis.shape[3]
    return pl.pallas_call(
        functools.partial(back_kernel, m),
        out_shape=jax.ShapeDtypeStruct((nz, cols, rows), BF16),
        in_specs=[SMEM] + [VMEM] * 6,
        out_specs=VMEM,
        scratch_shapes=[pltpu.VMEM((cols, rank), BF16)],
        compiler_params=PARAMS,
        cost_estimate=cost(2 * nz * rows * cols * rank, 3 * 2**20),
        name="back",
    )(at, basis, w, *blocks)


def place_kernel(m, spots, at_ref, *refs):
    n = len(spots)
    blocks, out_ref, sems = refs[:n], refs[-2], refs[-1]
    x, core = at_ref[0], at_ref[1]
    copies = []
    for i, (dx, across, row) in enumerate(spots):
        rows, width = blocks[i].shape
        owner = lax.rem(x + dx, 4) * 2 + (1 - core if across else core)
        start = pl.multiple_of(owner * width, 128)
        copies.append(
            pltpu.make_async_copy(
                blocks[i], out_ref.at[m, pl.ds(row, rows), pl.ds(start, width)], sems.at[i]
            )
        )
    for copy in copies:
        copy.start()
    for copy in copies:
        copy.wait()


def place(whole, shape, m, at, items):
    spots = [item[1:] for item in items]
    blocks = [item[0] for item in items]
    n = len(blocks)
    given = () if whole is None else (whole,)
    size = sum(2 * 2 * b.size for b in blocks)
    return pl.pallas_call(
        functools.partial(place_kernel, m, spots),
        out_shape=jax.ShapeDtypeStruct(shape, BF16),
        in_specs=[SMEM] + [VMEM] * n + [ANY] * len(given),
        out_specs=ANY,
        scratch_shapes=[pltpu.SemaphoreType.DMA((n,))],
        input_output_aliases={} if whole is None else {n + 1: 0},
        compiler_params=PARAMS,
        cost_estimate=cost(2e9, size),
        name="place",
    )(at, *blocks, *given)


def step(grads, basis, moment1, moment2, weights):
    x, core = lax.axis_index("x"), lax.axis_index("core")
    y, z = lax.axis_index("y"), lax.axis_index("z")
    nx, nc, ny, nz = (lax.axis_size(a) for a in ("x", "core", "y", "z"))
    mats, rows, cols = grads.shape
    rank = basis.shape[2]
    at = jnp.stack([x, core, y, z])

    held = exchange(pieces(at, grads, basis, nz), "z")
    sent = pack(grads, nz)
    mine = exchange(sent, "z")
    w = pack(weights, nz)
    state = pack_state(at, moment1, moment2, nz)
    own = jnp.stack([held] + [shift(held, "x", k) for k in range(1, nx)])
    peer = shift(own, "core", 1)
    state = [state[0]] + [shift(state[k], "z", k) for k in range(1, nz)]
    w = exchange(before(mine, w), "z")

    gathered, parts = project(at, mine, own, peer, rank, ny)
    parts = [parts[0]] + [shift(parts[k], "y", k) for k in range(1, ny)]
    summed = (parts[0] + parts[1]) + (parts[2] + parts[3])
    news, update = moments(at, summed, state)
    updates = [update] + [shift(update, "y", k) for k in range(1, ny)]
    fresh = [exchange(back(m, at, gathered, w, updates), "z") for m in range(mats)]
    news = unpack_state(exchange(before(fresh[-1], news), "z"))
    fresh = [jnp.swapaxes(f.reshape(cols, rows), 0, 1) for f in fresh]

    half = rows // 2
    shape = (mats, rows, cols * nx * nc)

    def put(whole, m, items):
        there = [(shift(b, "core", 1), dx, True, row) for b, dx, row in items]
        here = [(b, dx, False, row) for b, dx, row in items]
        return place(whole, shape, m, at, here + there)

    near = [(shift(f, "x", 1), shift(f, "x", -1)) for f in fresh]
    whole = put(None, 0, [(fresh[0], 0, 0)])
    whole = put(whole, 0, [(near[0][0], 3, 0), (near[0][1], 1, 0)])
    for m in range(mats):
        left, right = near[m]
        if m:
            whole, left, right = lax.optimization_barrier((whole, left, right))
            whole = put(whole, m, [(fresh[m], 0, 0)])
            whole = put(whole, m, [(left, 3, 0), (right, 1, 0)])
        top, low = shift(left[:half], "x", 1), shift(right[half:], "x", -1)
        if m:
            whole, top, low = lax.optimization_barrier((whole, top, low))
        whole = put(whole, m, [(top, 2, 0), (low, 2, half)])
    return (whole, news[0], news[1])


def solution(mesh):
    finer = Mesh(mesh.devices.reshape(4, 2, 4, 8), ("x", "core", "y", "z"))
    dp, rows = ("x", "core"), ("y", "z")
    in_specs = (
        P(None, rows, dp),
        P(None, rows, None),
        P(None, rows, dp),
        P(None, rows, dp),
        P(None, rows, dp),
    )
    out_specs = (P(None, rows, None), P(None, rows, dp), P(None, rows, dp))
    return jax.shard_map(step, mesh=finer, in_specs=in_specs, out_specs=out_specs, check_vma=False)
```

```python
import functools
import math

import jax
import jax.numpy as jnp
from jax import lax
from jax.experimental import pallas as pl
from jax.experimental.pallas import tpu as pltpu
from jax.sharding import Mesh
from jax.sharding import PartitionSpec as P


D = 4096
FF = 14336
MATS = 2
STEP = 10
F32 = jnp.float32
BF16 = jnp.bfloat16
VMEM = pl.BlockSpec(memory_space=pltpu.VMEM)
SMEM = pl.BlockSpec(memory_space=pltpu.SMEM)
ANY = pl.BlockSpec(memory_space=pl.ANY)
PARAMS = pltpu.CompilerParams(vmem_limit_bytes=8 * 2**20)


def shift(v, axis, k):
    n = lax.axis_size(axis)
    return lax.ppermute(v, axis, [(i, (i + k) % n) for i in range(n)])


def exchange(v, axis):
    return lax.all_to_all(v, axis, split_axis=0, concat_axis=0, tiled=True)


def cost(flops, size):
    return pl.CostEstimate(flops=int(flops), bytes_accessed=int(size), transcendentals=0)


def before(first, second):
    return lax.optimization_barrier((first, second))[1]


def pack_kernel(v_ref, out_ref):
    nz, _, cols, _ = out_ref.shape
    for m in range(MATS):
        turned = jnp.transpose(v_ref[m])
        for z in range(nz):
            out_ref[z, m] = turned[z * cols : (z + 1) * cols]


def pack(v, nz):
    mats, rows, cols = v.shape
    return pl.pallas_call(
        pack_kernel,
        out_shape=jax.ShapeDtypeStruct((nz, mats, cols // nz, rows), BF16),
        in_specs=[VMEM],
        out_specs=VMEM,
        compiler_params=PARAMS,
        cost_estimate=cost(2e9, 2 * 2**20),
        name="pack",
    )(v)


def pieces_kernel(at_ref, v_ref, basis_ref, out_ref):
    nz, size, width = out_ref.shape
    part = basis_ref.shape[1] // 8
    start = pl.multiple_of((at_ref[0] * 2 + at_ref[1]) * part, part)
    total = None
    for m in range(MATS):
        wide = v_ref[m].astype(F32)
        squares = jnp.sum(wide * wide, axis=0, keepdims=True)
        total = squares if total is None else total + squares
        piece = basis_ref[m, pl.ds(start, part)]
        count = piece.shape[1] // width
        for k in range(count):
            low = (m * count + k) * part
            for z in range(nz):
                out_ref[z, low : low + part] = piece[:, k * width : (k + 1) * width]
    total = jnp.sum(total, axis=1, keepdims=True)
    high = total.astype(BF16).astype(F32)
    middle = (total - high).astype(BF16).astype(F32)
    low = total - high - middle
    row = lax.broadcasted_iota(jnp.int32, (part, width), 0)
    tile = jnp.where(row == 0, high, jnp.where(row == 1, middle, jnp.where(row == 2, low, 0.0)))
    for z in range(nz):
        out_ref[z, size - part :] = tile.astype(BF16)


def pieces(at, v, basis, nz):
    mats, rows, rank = basis.shape
    part, width = rows // 8, 128
    return pl.pallas_call(
        pieces_kernel,
        out_shape=jax.ShapeDtypeStruct((nz, mats * part * rank // width + part, width), BF16),
        in_specs=[SMEM, VMEM, VMEM],
        out_specs=VMEM,
        compiler_params=PARAMS,
        cost_estimate=cost(2e9, 2**20),
        name="pieces",
    )(at, v, basis)


def pack_state_kernel(at_ref, one_ref, two_ref, *refs):
    outs, held_ref = refs[:-1], refs[-1]
    nz, _, cols = held_ref.shape
    ranks = one_ref.shape[1]
    for k, ref in enumerate((one_ref, two_ref)):
        for m in range(MATS):
            low = (k * MATS + m) * ranks
            for z in range(nz):
                held_ref[z, low : low + ranks] = ref[m, :, z * cols : (z + 1) * cols]
    for d in range(nz):
        outs[d][...] = held_ref[lax.rem(at_ref[3] + d, nz)]


def pack_state(at, one, two, nz):
    mats, ranks, cols = one.shape
    size = (2 * mats * ranks, cols // nz)
    return pl.pallas_call(
        pack_state_kernel,
        out_shape=[jax.ShapeDtypeStruct(size, F32)] * nz,
        in_specs=[SMEM, VMEM, VMEM],
        out_specs=[VMEM] * nz,
        scratch_shapes=[pltpu.VMEM((nz, *size), F32)],
        compiler_params=PARAMS,
        cost_estimate=cost(2e9, 2**20),
        name="pack_state",
    )(at, one, two)


def unpack_state_kernel(in_ref, one_ref, two_ref):
    nz, _, _ = in_ref.shape
    ranks = one_ref.shape[1]
    for k, ref in enumerate((one_ref, two_ref)):
        for m in range(MATS):
            low = (k * MATS + m) * ranks
            ref[m] = jnp.concatenate([in_ref[z, low : low + ranks] for z in range(nz)], axis=1)


def unpack_state(held):
    nz, kinds, cols = held.shape
    shape = jax.ShapeDtypeStruct((MATS, kinds // (2 * MATS), nz * cols), F32)
    return pl.pallas_call(
        unpack_state_kernel,
        out_shape=[shape, shape],
        in_specs=[VMEM],
        out_specs=[VMEM] * 2,
        compiler_params=PARAMS,
        cost_estimate=cost(2e9, 2**20),
        name="unpack_state",
    )(held)


def project_kernel(at_ref, g_ref, own_ref, peer_ref, basis_ref, *refs):
    outs, total_ref = refs[:-1], refs[-1]
    x, core, y = (at_ref[i] for i in range(3))
    nx, nz, size, width = own_ref.shape
    rank = basis_ref.shape[3]
    part = basis_ref.shape[2] // (2 * nx)
    count = rank // width
    cols = g_ref.shape[2]
    ny = len(outs)

    def gather(z, _):
        for m in range(MATS):
            for xa in range(nx):
                d = lax.rem(x - xa + nx, nx)
                for k in range(count):
                    low = (m * count + k) * part
                    ours, theirs = own_ref[d, z, low : low + part], peer_ref[d, z, low : low + part]
                    at = 2 * xa * part
                    lanes = slice(k * width, (k + 1) * width)
                    basis_ref[m, z, at : at + part, lanes] = jnp.where(core == 0, ours, theirs)
                    basis_ref[m, z, at + part : at + 2 * part, lanes] = jnp.where(
                        core == 0, theirs, ours
                    )
        return 0

    lax.fori_loop(0, nz, gather, 0)

    def multiply(m, _):
        left = jnp.concatenate([g_ref[z, m] for z in range(nz)], axis=1)
        right = basis_ref[m].reshape(left.shape[1], -1)
        total_ref[m] = jnp.dot(left, right, preferred_element_type=F32)
        return 0

    lax.fori_loop(0, MATS, multiply, 0)
    squares = jnp.zeros((part, width), F32)
    for ref in (own_ref, peer_ref):
        for d in range(nx):
            for z in range(nz):
                squares = squares + ref[d, z, size - part :].astype(F32)
    squares = jnp.sum(squares, axis=0, keepdims=True)
    for d in range(ny):
        start = pl.multiple_of(lax.rem(y + d, ny) * width, width)
        outs[d][:, :cols] = total_ref[:, :, pl.ds(start, width)]
        for m in range(MATS):
            outs[d][m, cols:] = jnp.broadcast_to(squares, (8, width))


def project(at, g, own, peer, rank, parts):
    nz, mats, cols, rows = g.shape
    basis, *out = pl.pallas_call(
        project_kernel,
        out_shape=[jax.ShapeDtypeStruct((mats, nz, rows, rank), BF16)]
        + [jax.ShapeDtypeStruct((mats, cols + 8, rank // parts), F32)] * parts,
        in_specs=[SMEM] + [VMEM] * 3,
        out_specs=[VMEM] * (1 + parts),
        scratch_shapes=[pltpu.VMEM((mats, cols, rank), F32)],
        compiler_params=PARAMS,
        cost_estimate=cost(2 * mats * nz * cols * rows * rank, 4 * 2**20),
        name="project",
    )(at, g, own, peer)
    return basis, out


def moments_kernel(at_ref, sum_ref, *refs):
    held, new_ref, update_ref, held_ref = refs[:-3], refs[-3], refs[-2], refs[-1]
    nz, kinds, cols = held_ref.shape
    ranks = kinds // (2 * MATS)
    for d in range(nz):
        held_ref[lax.rem(at_ref[3] - d + nz, nz)] = held[d][...]
    limit = 1.0 * math.sqrt(MATS * D * FF)
    scale = limit / jnp.maximum(jnp.sqrt(sum_ref[0, cols : cols + 1, 0:1]), limit)
    first_bias_correction = 1.0 - 0.9**STEP
    second_fix = 1.0 - 0.999**STEP
    spare = 256 - cols
    for m in range(MATS):
        one, two = (slice(k * ranks, (k + 1) * ranks) for k in (m, MATS + m))
        summed = sum_ref[m, :cols]
        padded = jnp.concatenate([summed, jnp.zeros((spare, summed.shape[1]), F32)], axis=0)
        scaled = scale * jnp.transpose(padded)[:, :cols]
        first = 0.9 * held_ref[:, one].reshape(nz * ranks, cols) + 0.1 * scaled
        second = 0.999 * held_ref[:, two].reshape(nz * ranks, cols) + 0.001 * scaled * scaled
        new_ref[:, one] = first.reshape(nz, ranks, cols)
        new_ref[:, two] = second.reshape(nz, ranks, cols)
        update = first / first_bias_correction / (jnp.sqrt(second / second_fix) + 1e-08)
        wide = jnp.concatenate([update, jnp.zeros((update.shape[0], spare), F32)], axis=1)
        update_ref[m] = jnp.transpose(wide)[:cols].astype(BF16)


def moments(at, summed, held):
    nz = len(held)
    kinds, cols = held[0].shape
    ranks = kinds // (2 * MATS)
    return pl.pallas_call(
        moments_kernel,
        out_shape=[
            jax.ShapeDtypeStruct((nz, kinds, cols), F32),
            jax.ShapeDtypeStruct((MATS, cols, nz * ranks), BF16),
        ],
        in_specs=[SMEM] + [VMEM] * (1 + nz),
        out_specs=[VMEM] * 2,
        scratch_shapes=[pltpu.VMEM((nz, kinds, cols), F32)],
        compiler_params=PARAMS,
        cost_estimate=cost(2e9, 2 * 2**20),
        name="moments",
    )(at, summed, *held)


def back_kernel(m, at_ref, basis_ref, w_ref, u0, u1, u2, u3, *refs):
    outs, whole_ref = refs[:-1], refs[-1]
    y, here = at_ref[2], at_ref[3]
    nz = basis_ref.shape[1]
    width = u0.shape[2]
    blocks = (u0, u1, u2, u3)
    n = len(blocks)
    for d in range(n):
        start = pl.multiple_of(lax.rem(y - d + n, n) * width, width)
        whole_ref[:, pl.ds(start, width)] = blocks[d][m]

    def rows(z):
        product = lax.dot_general(
            whole_ref[...], basis_ref[m, z], (((1,), (1,)), ((), ())), preferred_element_type=F32
        )
        return (w_ref[z, m].astype(F32) - 0.5 * product).astype(BF16)

    if len(outs) == 1:

        def store(z, _):
            outs[0][z] = rows(z)
            return 0

        lax.fori_loop(0, nz, store, 0)
    else:
        for d in range(nz):
            outs[d][...] = rows(lax.rem(here + d, nz))


def back(m, at, basis, w, blocks, apart):
    nz, _, cols, rows = w.shape
    rank = basis.shape[3]
    shapes = [(cols, rows)] * nz if apart else [(nz, cols, rows)]
    return pl.pallas_call(
        functools.partial(back_kernel, m),
        out_shape=[jax.ShapeDtypeStruct(shape, BF16) for shape in shapes],
        in_specs=[SMEM] + [VMEM] * 6,
        out_specs=[VMEM] * len(shapes),
        scratch_shapes=[pltpu.VMEM((cols, rank), BF16)],
        compiler_params=PARAMS,
        cost_estimate=cost(2 * nz * rows * cols * rank, 3 * 2**20),
        name="back",
    )(at, basis, w, *blocks)


def turn_kernel(at_ref, *refs):
    blocks, out_ref, held_ref = refs[:-2], refs[-2], refs[-1]
    nz, cols, rows = held_ref.shape
    for d in range(nz):
        held_ref[lax.rem(at_ref[3] - d + nz, nz)] = blocks[d][...]
    out_ref[...] = jnp.transpose(held_ref[...].reshape(nz * cols, rows))


def turn(at, blocks):
    nz = len(blocks)
    cols, rows = blocks[0].shape
    return pl.pallas_call(
        turn_kernel,
        out_shape=jax.ShapeDtypeStruct((rows, nz * cols), BF16),
        in_specs=[SMEM] + [VMEM] * nz,
        out_specs=VMEM,
        scratch_shapes=[pltpu.VMEM((nz, cols, rows), BF16)],
        compiler_params=PARAMS,
        cost_estimate=cost(2e9, 2**20),
        name="turn",
    )(at, *blocks)


def place_kernel(m, spots, at_ref, *refs):
    n = len(spots)
    blocks, out_ref, sems = refs[:n], refs[-2], refs[-1]
    x, core = at_ref[0], at_ref[1]
    copies = []
    for i, (dx, across, row) in enumerate(spots):
        rows, width = blocks[i].shape
        owner = lax.rem(x + dx, 4) * 2 + (1 - core if across else core)
        start = pl.multiple_of(owner * width, 128)
        copies.append(
            pltpu.make_async_copy(
                blocks[i], out_ref.at[m, pl.ds(row, rows), pl.ds(start, width)], sems.at[i]
            )
        )
    for copy in copies:
        copy.start()
    for copy in copies:
        copy.wait()


def place(whole, shape, m, at, items):
    spots = [item[1:] for item in items]
    blocks = [item[0] for item in items]
    n = len(blocks)
    given = () if whole is None else (whole,)
    size = sum(2 * 2 * b.size for b in blocks)
    return pl.pallas_call(
        functools.partial(place_kernel, m, spots),
        out_shape=jax.ShapeDtypeStruct(shape, BF16),
        in_specs=[SMEM] + [VMEM] * n + [ANY] * len(given),
        out_specs=ANY,
        scratch_shapes=[pltpu.SemaphoreType.DMA((n,))],
        input_output_aliases={} if whole is None else {n + 1: 0},
        compiler_params=PARAMS,
        cost_estimate=cost(2e9, size),
        name="place",
    )(at, *blocks, *given)


def step(grads, basis, moment1, moment2, weights):
    x, core = lax.axis_index("x"), lax.axis_index("core")
    y, z = lax.axis_index("y"), lax.axis_index("z")
    nx, nc, ny, nz = (lax.axis_size(a) for a in ("x", "core", "y", "z"))
    mats, rows, cols = grads.shape
    rank = basis.shape[2]
    at = jnp.stack([x, core, y, z])

    held = exchange(pieces(at, grads, basis, nz), "z")
    sent = pack(grads, nz)
    mine = exchange(sent, "z")
    w = pack(weights, nz)
    state = pack_state(at, moment1, moment2, nz)
    own = jnp.stack([held] + [shift(held, "x", k) for k in range(1, nx)])
    peer = shift(own, "core", 1)
    state = [state[0]] + [shift(state[k], "z", k) for k in range(1, nz)]
    w = exchange(before(mine, w), "z")

    gathered, parts = project(at, mine, own, peer, rank, ny)
    parts = [parts[0]] + [shift(parts[k], "y", k) for k in range(1, ny)]
    summed = (parts[0] + parts[1]) + (parts[2] + parts[3])
    news, update = moments(at, summed, state)
    updates = [update] + [shift(update, "y", k) for k in range(1, ny)]
    whole_block = back(0, at, gathered, w, updates, False)[0]
    whole_block = exchange(whole_block, "z")
    blocks = back(1, at, gathered, w, updates, True)
    blocks = [blocks[0]] + [shift(blocks[k], "z", k) for k in range(1, nz)]
    fresh = [jnp.swapaxes(whole_block.reshape(cols, rows), 0, 1), turn(at, blocks)]
    news = exchange(before(whole_block, news), "z")
    news = unpack_state(news)

    half = rows // 2
    shape = (mats, rows, cols * nx * nc)

    def put(whole, m, items):
        there = [(shift(b, "core", 1), dx, True, row) for b, dx, row in items]
        here = [(b, dx, False, row) for b, dx, row in items]
        return place(whole, shape, m, at, here + there)

    near = []
    for f in fresh:
        near.append((shift(f, "x", 1), shift(f, "x", -1)))
    whole = put(None, 0, [(fresh[0], 0, 0)])
    whole = put(whole, 0, [(near[0][0], 3, 0), (near[0][1], 1, 0)])
    for m in range(mats):
        left, right = near[m]
        if m:
            whole, left, right = lax.optimization_barrier((whole, left, right))
            whole = put(whole, m, [(fresh[m], 0, 0)])
            whole = put(whole, m, [(left, 3, 0), (right, 1, 0)])
        top, low = shift(left[:half], "x", 1), shift(right[half:], "x", -1)
        if m:
            whole, top, low = lax.optimization_barrier((whole, top, low))
        whole = put(whole, m, [(top, 2, 0), (low, 2, half)])
    return (whole, news[0], news[1])


def solution(mesh):
    finer = Mesh(mesh.devices.reshape(4, 2, 4, 8), ("x", "core", "y", "z"))
    dp, rows = ("x", "core"), ("y", "z")
    in_specs = (
        P(None, rows, dp),
        P(None, rows, None),
        P(None, rows, dp),
        P(None, rows, dp),
        P(None, rows, dp),
    )
    out_specs = (P(None, rows, None), P(None, rows, dp), P(None, rows, dp))
    return jax.shard_map(step, mesh=finer, in_specs=in_specs, out_specs=out_specs, check_vma=False)
```

```python
import functools
import math

import jax
import jax.numpy as jnp
from jax import lax
from jax.experimental import pallas as pl
from jax.experimental.pallas import tpu as pltpu
from jax.sharding import Mesh
from jax.sharding import PartitionSpec as P


D = 4096
FF = 14336
MATS = 2
STEP = 10
F32 = jnp.float32
BF16 = jnp.bfloat16
VMEM = pl.BlockSpec(memory_space=pltpu.VMEM)
SMEM = pl.BlockSpec(memory_space=pltpu.SMEM)
ANY = pl.BlockSpec(memory_space=pl.ANY)
PARAMS = pltpu.CompilerParams(vmem_limit_bytes=8 * 2**20)


def shift(v, axis, k):
    n = lax.axis_size(axis)
    return lax.ppermute(v, axis, [(i, (i + k) % n) for i in range(n)])


def exchange(v, axis):
    return lax.all_to_all(v, axis, split_axis=0, concat_axis=0, tiled=True)


def cost(flops, size):
    return pl.CostEstimate(flops=int(flops), bytes_accessed=int(size), transcendentals=0)


def before(first, second):
    return lax.optimization_barrier((first, second))[1]


def pack_kernel(v_ref, out_ref):
    nz, _, cols, _ = out_ref.shape
    for m in range(MATS):
        turned = jnp.transpose(v_ref[m])
        for z in range(nz):
            out_ref[z, m] = turned[z * cols : (z + 1) * cols]


def pack(v, nz):
    mats, rows, cols = v.shape
    return pl.pallas_call(
        pack_kernel,
        out_shape=jax.ShapeDtypeStruct((nz, mats, cols // nz, rows), BF16),
        in_specs=[VMEM],
        out_specs=VMEM,
        compiler_params=PARAMS,
        cost_estimate=cost(2e9, 2 * 2**20),
        name="pack",
    )(v)


def pieces_kernel(at_ref, v_ref, basis_ref, out_ref):
    nz, size, width = out_ref.shape
    part = basis_ref.shape[1] // 8
    start = pl.multiple_of((at_ref[0] * 2 + at_ref[1]) * part, part)
    total = None
    for m in range(MATS):
        wide = v_ref[m].astype(F32)
        squares = jnp.sum(wide * wide, axis=0, keepdims=True)
        total = squares if total is None else total + squares
        piece = basis_ref[m, pl.ds(start, part)]
        count = piece.shape[1] // width
        for k in range(count):
            low = (m * count + k) * part
            for z in range(nz):
                out_ref[z, low : low + part] = piece[:, k * width : (k + 1) * width]
    total = jnp.sum(total, axis=1, keepdims=True)
    high = total.astype(BF16).astype(F32)
    middle = (total - high).astype(BF16).astype(F32)
    low = total - high - middle
    row = lax.broadcasted_iota(jnp.int32, (part, width), 0)
    tile = jnp.where(row == 0, high, jnp.where(row == 1, middle, jnp.where(row == 2, low, 0.0)))
    for z in range(nz):
        out_ref[z, size - part :] = tile.astype(BF16)


def pieces(at, v, basis, nz):
    mats, rows, rank = basis.shape
    part, width = rows // 8, 128
    return pl.pallas_call(
        pieces_kernel,
        out_shape=jax.ShapeDtypeStruct((nz, mats * part * rank // width + part, width), BF16),
        in_specs=[SMEM, VMEM, VMEM],
        out_specs=VMEM,
        compiler_params=PARAMS,
        cost_estimate=cost(2e9, 2**20),
        name="pieces",
    )(at, v, basis)


def pack_state_kernel(at_ref, one_ref, two_ref, *refs):
    outs, held_ref = refs[:-1], refs[-1]
    nz, _, cols = held_ref.shape
    ranks = one_ref.shape[1]
    for k, ref in enumerate((one_ref, two_ref)):
        for m in range(MATS):
            low = (k * MATS + m) * ranks
            for z in range(nz):
                held_ref[z, low : low + ranks] = ref[m, :, z * cols : (z + 1) * cols]
    for d in range(nz):
        outs[d][...] = held_ref[lax.rem(at_ref[3] + d, nz)]


def pack_state(at, one, two, nz):
    mats, ranks, cols = one.shape
    size = (2 * mats * ranks, cols // nz)
    return pl.pallas_call(
        pack_state_kernel,
        out_shape=[jax.ShapeDtypeStruct(size, F32)] * nz,
        in_specs=[SMEM, VMEM, VMEM],
        out_specs=[VMEM] * nz,
        scratch_shapes=[pltpu.VMEM((nz, *size), F32)],
        compiler_params=PARAMS,
        cost_estimate=cost(2e9, 2**20),
        name="pack_state",
    )(at, one, two)


def unpack_state_kernel(in_ref, one_ref, two_ref):
    nz, _, _ = in_ref.shape
    ranks = one_ref.shape[1]
    for k, ref in enumerate((one_ref, two_ref)):
        for m in range(MATS):
            low = (k * MATS + m) * ranks
            ref[m] = jnp.concatenate([in_ref[z, low : low + ranks] for z in range(nz)], axis=1)


def unpack_state(held):
    nz, kinds, cols = held.shape
    shape = jax.ShapeDtypeStruct((MATS, kinds // (2 * MATS), nz * cols), F32)
    return pl.pallas_call(
        unpack_state_kernel,
        out_shape=[shape, shape],
        in_specs=[VMEM],
        out_specs=[VMEM] * 2,
        compiler_params=PARAMS,
        cost_estimate=cost(2e9, 2**20),
        name="unpack_state",
    )(held)


def project_kernel(at_ref, g_ref, own_ref, peer_ref, basis_ref, *refs):
    outs, total_ref = refs[:-1], refs[-1]
    x, core, y = (at_ref[i] for i in range(3))
    nx, nz, size, width = own_ref.shape
    rank = basis_ref.shape[3]
    part = basis_ref.shape[2] // (2 * nx)
    count = rank // width
    cols = g_ref.shape[2]
    ny = len(outs)

    def gather(z, _):
        for m in range(MATS):
            for xa in range(nx):
                d = lax.rem(x - xa + nx, nx)
                for k in range(count):
                    low = (m * count + k) * part
                    ours, theirs = own_ref[d, z, low : low + part], peer_ref[d, z, low : low + part]
                    at = 2 * xa * part
                    lanes = slice(k * width, (k + 1) * width)
                    basis_ref[m, z, at : at + part, lanes] = jnp.where(core == 0, ours, theirs)
                    basis_ref[m, z, at + part : at + 2 * part, lanes] = jnp.where(
                        core == 0, theirs, ours
                    )
        return 0

    lax.fori_loop(0, nz, gather, 0)

    def multiply(m, _):
        left = jnp.concatenate([g_ref[z, m] for z in range(nz)], axis=1)
        right = basis_ref[m].reshape(left.shape[1], -1)
        total_ref[m] = jnp.dot(left, right, preferred_element_type=F32)
        return 0

    lax.fori_loop(0, MATS, multiply, 0)
    squares = jnp.zeros((part, width), F32)
    for ref in (own_ref, peer_ref):
        for d in range(nx):
            for z in range(nz):
                squares = squares + ref[d, z, size - part :].astype(F32)
    squares = jnp.sum(squares, axis=0, keepdims=True)
    for d in range(ny):
        start = pl.multiple_of(lax.rem(y + d, ny) * width, width)
        outs[d][:, :cols] = total_ref[:, :, pl.ds(start, width)]
        for m in range(MATS):
            outs[d][m, cols:] = jnp.broadcast_to(squares, (8, width))


def project(at, g, own, peer, rank, parts):
    nz, mats, cols, rows = g.shape
    basis, *out = pl.pallas_call(
        project_kernel,
        out_shape=[jax.ShapeDtypeStruct((mats, nz, rows, rank), BF16)]
        + [jax.ShapeDtypeStruct((mats, cols + 8, rank // parts), F32)] * parts,
        in_specs=[SMEM] + [VMEM] * 3,
        out_specs=[VMEM] * (1 + parts),
        scratch_shapes=[pltpu.VMEM((mats, cols, rank), F32)],
        compiler_params=PARAMS,
        cost_estimate=cost(2 * mats * nz * cols * rows * rank, 4 * 2**20),
        name="project",
    )(at, g, own, peer)
    return basis, out


def moments_kernel(at_ref, sum_ref, *refs):
    held, new_ref, update_ref, held_ref = refs[:-3], refs[-3], refs[-2], refs[-1]
    nz, kinds, cols = held_ref.shape
    ranks = kinds // (2 * MATS)
    for d in range(nz):
        held_ref[lax.rem(at_ref[3] - d + nz, nz)] = held[d][...]
    limit = 1.0 * math.sqrt(MATS * D * FF)
    scale = limit / jnp.maximum(jnp.sqrt(sum_ref[0, cols : cols + 1, 0:1]), limit)
    first_bias_correction = 1.0 - 0.9**STEP
    second_fix = 1.0 - 0.999**STEP
    spare = 256 - cols
    for m in range(MATS):
        one, two = (slice(k * ranks, (k + 1) * ranks) for k in (m, MATS + m))
        summed = sum_ref[m, :cols]
        padded = jnp.concatenate([summed, jnp.zeros((spare, summed.shape[1]), F32)], axis=0)
        scaled = scale * jnp.transpose(padded)[:, :cols]
        first = 0.9 * held_ref[:, one].reshape(nz * ranks, cols) + 0.1 * scaled
        second = 0.999 * held_ref[:, two].reshape(nz * ranks, cols) + 0.001 * scaled * scaled
        new_ref[:, one] = first.reshape(nz, ranks, cols)
        new_ref[:, two] = second.reshape(nz, ranks, cols)
        update = first / first_bias_correction / (jnp.sqrt(second / second_fix) + 1e-08)
        wide = jnp.concatenate([update, jnp.zeros((update.shape[0], spare), F32)], axis=1)
        update_ref[m] = jnp.transpose(wide)[:cols].astype(BF16)


def moments(at, summed, held):
    nz = len(held)
    kinds, cols = held[0].shape
    ranks = kinds // (2 * MATS)
    return pl.pallas_call(
        moments_kernel,
        out_shape=[
            jax.ShapeDtypeStruct((nz, kinds, cols), F32),
            jax.ShapeDtypeStruct((MATS, cols, nz * ranks), BF16),
        ],
        in_specs=[SMEM] + [VMEM] * (1 + nz),
        out_specs=[VMEM] * 2,
        scratch_shapes=[pltpu.VMEM((nz, kinds, cols), F32)],
        compiler_params=PARAMS,
        cost_estimate=cost(2e9, 2 * 2**20),
        name="moments",
    )(at, summed, *held)


def back_kernel(m, at_ref, basis_ref, w_ref, u0, u1, u2, u3, *refs):
    outs, whole_ref = refs[:-1], refs[-1]
    y, here = at_ref[2], at_ref[3]
    nz = basis_ref.shape[1]
    width = u0.shape[2]
    blocks = (u0, u1, u2, u3)
    n = len(blocks)
    for d in range(n):
        start = pl.multiple_of(lax.rem(y - d + n, n) * width, width)
        whole_ref[:, pl.ds(start, width)] = blocks[d][m]

    def rows(z):
        product = lax.dot_general(
            whole_ref[...], basis_ref[m, z], (((1,), (1,)), ((), ())), preferred_element_type=F32
        )
        return (w_ref[z, m].astype(F32) - 0.5 * product).astype(BF16)

    if len(outs) == 1:

        def store(z, _):
            outs[0][z] = rows(z)
            return 0

        lax.fori_loop(0, nz, store, 0)
    else:
        for d in range(nz):
            outs[d][...] = rows(lax.rem(here + d, nz))


def back(m, at, basis, w, blocks, apart):
    nz, _, cols, rows = w.shape
    rank = basis.shape[3]
    shapes = [(cols, rows)] * nz if apart else [(nz, cols, rows)]
    return pl.pallas_call(
        functools.partial(back_kernel, m),
        out_shape=[jax.ShapeDtypeStruct(shape, BF16) for shape in shapes],
        in_specs=[SMEM] + [VMEM] * 6,
        out_specs=[VMEM] * len(shapes),
        scratch_shapes=[pltpu.VMEM((cols, rank), BF16)],
        compiler_params=PARAMS,
        cost_estimate=cost(2 * nz * rows * cols * rank, 3 * 2**20),
        name="back",
    )(at, basis, w, *blocks)


def turn_kernel(at_ref, *refs):
    blocks, out_ref, held_ref = refs[:-2], refs[-2], refs[-1]
    nz, cols, rows = held_ref.shape
    for d in range(nz):
        held_ref[lax.rem(at_ref[3] - d + nz, nz)] = blocks[d][...]
    out_ref[...] = jnp.transpose(held_ref[...].reshape(nz * cols, rows))


def turn(at, blocks):
    nz = len(blocks)
    cols, rows = blocks[0].shape
    return pl.pallas_call(
        turn_kernel,
        out_shape=jax.ShapeDtypeStruct((rows, nz * cols), BF16),
        in_specs=[SMEM] + [VMEM] * nz,
        out_specs=VMEM,
        scratch_shapes=[pltpu.VMEM((nz, cols, rows), BF16)],
        compiler_params=PARAMS,
        cost_estimate=cost(2e9, 2**20),
        name="turn",
    )(at, *blocks)


def place_kernel(m, spots, at_ref, *refs):
    n = len(spots)
    blocks, out_ref, sems = refs[:n], refs[-2], refs[-1]
    x, core = at_ref[0], at_ref[1]
    copies = []
    for i, (dx, across, row) in enumerate(spots):
        rows, width = blocks[i].shape
        owner = lax.rem(x + dx, 4) * 2 + (1 - core if across else core)
        start = pl.multiple_of(owner * width, 128)
        copies.append(
            pltpu.make_async_copy(
                blocks[i], out_ref.at[m, pl.ds(row, rows), pl.ds(start, width)], sems.at[i]
            )
        )
    for copy in copies:
        copy.start()
    for copy in copies:
        copy.wait()


def place(whole, shape, m, at, items):
    spots = [item[1:] for item in items]
    blocks = [item[0] for item in items]
    n = len(blocks)
    given = () if whole is None else (whole,)
    size = sum(2 * 2 * b.size for b in blocks)
    return pl.pallas_call(
        functools.partial(place_kernel, m, spots),
        out_shape=jax.ShapeDtypeStruct(shape, BF16),
        in_specs=[SMEM] + [VMEM] * n + [ANY] * len(given),
        out_specs=ANY,
        scratch_shapes=[pltpu.SemaphoreType.DMA((n,))],
        input_output_aliases={} if whole is None else {n + 1: 0},
        compiler_params=PARAMS,
        cost_estimate=cost(2e9, size),
        name="place",
    )(at, *blocks, *given)


def step(grads, basis, moment1, moment2, weights):
    x, core = lax.axis_index("x"), lax.axis_index("core")
    y, z = lax.axis_index("y"), lax.axis_index("z")
    nx, nc, ny, nz = (lax.axis_size(a) for a in ("x", "core", "y", "z"))
    mats, rows, cols = grads.shape
    rank = basis.shape[2]
    at = jnp.stack([x, core, y, z])

    held = exchange(pieces(at, grads, basis, nz), "z")
    sent = pack(grads, nz)
    mine = exchange(sent, "z")
    w = pack(weights, nz)
    state = pack_state(at, moment1, moment2, nz)
    own = jnp.stack([held] + [shift(held, "x", k) for k in range(1, nx)])
    peer = shift(own, "core", 1)
    state = [state[0]] + [shift(state[k], "z", k) for k in range(1, nz)]
    w = exchange(before(mine, w), "z")

    gathered, parts = project(at, mine, own, peer, rank, ny)
    parts = [parts[0]] + [shift(parts[k], "y", k) for k in range(1, ny)]
    summed = (parts[0] + parts[1]) + (parts[2] + parts[3])
    news, update = moments(at, summed, state)
    updates = [update] + [shift(update, "y", k) for k in range(1, ny)]
    whole_block = back(0, at, gathered, w, updates, False)[0]
    whole_block = exchange(whole_block, "z")
    blocks = back(1, at, gathered, w, updates, True)
    moved = [blocks[0]]
    for k in range(1, nz):
        moved.append(shift(blocks[k], "z", k))
    turned = turn(at, moved)
    fresh = [jnp.swapaxes(whole_block.reshape(cols, rows), 0, 1), turned]
    news = exchange(before(whole_block, news), "z")
    news = unpack_state(news)

    half = rows // 2
    shape = (mats, rows, cols * nx * nc)

    def put(whole, m, items):
        there = [(shift(b, "core", 1), dx, True, row) for b, dx, row in items]
        here = [(b, dx, False, row) for b, dx, row in items]
        return place(whole, shape, m, at, here + there)

    near = []
    for f in fresh:
        near.append((shift(f, "x", 1), shift(f, "x", -1)))

    def far(left, right):
        return shift(left[:half], "x", 1), shift(right[half:], "x", -1)

    def put_near(whole, m):
        whole = put(whole, m, [(fresh[m], 0, 0)])
        return put(whole, m, [(near[m][0], 3, 0), (near[m][1], 1, 0)])

    def put_far(whole, m, top, low):
        return put(whole, m, [(top, 2, 0), (low, 2, half)])

    first = far(*near[0])
    whole = put_near(None, 0)
    second = far(*near[1])
    whole = put_far(whole, 0, *first)
    whole = put_near(whole, 1)
    whole, *second = lax.optimization_barrier((whole, *second))
    whole = put_far(whole, 1, *second)
    return (whole, news[0], news[1])


def solution(mesh):
    finer = Mesh(mesh.devices.reshape(4, 2, 4, 8), ("x", "core", "y", "z"))
    dp, rows = ("x", "core"), ("y", "z")
    in_specs = (
        P(None, rows, dp),
        P(None, rows, None),
        P(None, rows, dp),
        P(None, rows, dp),
        P(None, rows, dp),
    )
    out_specs = (P(None, rows, None), P(None, rows, dp), P(None, rows, dp))
    return jax.shard_map(step, mesh=finer, in_specs=in_specs, out_specs=out_specs, check_vma=False)
```

```python
import functools
import math

import jax
import jax.numpy as jnp
from jax import lax
from jax.experimental import pallas as pl
from jax.experimental.pallas import tpu as pltpu
from jax.sharding import Mesh
from jax.sharding import PartitionSpec as P


D = 4096
FF = 14336
MATS = 2
STEP = 10
F32 = jnp.float32
BF16 = jnp.bfloat16
VMEM = pl.BlockSpec(memory_space=pltpu.VMEM)
SMEM = pl.BlockSpec(memory_space=pltpu.SMEM)
ANY = pl.BlockSpec(memory_space=pl.ANY)
PARAMS = pltpu.CompilerParams(vmem_limit_bytes=8 * 2**20)


def shift(v, axis, k):
    n = lax.axis_size(axis)
    return lax.ppermute(v, axis, [(i, (i + k) % n) for i in range(n)])


def exchange(v, axis):
    return lax.all_to_all(v, axis, split_axis=0, concat_axis=0, tiled=True)


def cost(flops, size):
    return pl.CostEstimate(flops=int(flops), bytes_accessed=int(size), transcendentals=0)


def before(first, second):
    return lax.optimization_barrier((first, second))[1]


def pack_kernel(v_ref, out_ref):
    nz, _, cols, _ = out_ref.shape
    for m in range(MATS):
        turned = jnp.transpose(v_ref[m])
        for z in range(nz):
            out_ref[z, m] = turned[z * cols : (z + 1) * cols]


def pack(v, nz):
    mats, rows, cols = v.shape
    return pl.pallas_call(
        pack_kernel,
        out_shape=jax.ShapeDtypeStruct((nz, mats, cols // nz, rows), BF16),
        in_specs=[VMEM],
        out_specs=VMEM,
        compiler_params=PARAMS,
        cost_estimate=cost(2e9, 2 * 2**20),
        name="pack",
    )(v)


def pieces_kernel(at_ref, v_ref, basis_ref, out_ref):
    nz, size, width = out_ref.shape
    part = basis_ref.shape[1] // 8
    start = pl.multiple_of((at_ref[0] * 2 + at_ref[1]) * part, part)
    total = None
    for m in range(MATS):
        wide = v_ref[m].astype(F32)
        squares = jnp.sum(wide * wide, axis=0, keepdims=True)
        total = squares if total is None else total + squares
        piece = basis_ref[m, pl.ds(start, part)]
        count = piece.shape[1] // width
        for k in range(count):
            low = (m * count + k) * part
            for z in range(nz):
                out_ref[z, low : low + part] = piece[:, k * width : (k + 1) * width]
    total = jnp.sum(total, axis=1, keepdims=True)
    high = total.astype(BF16).astype(F32)
    middle = (total - high).astype(BF16).astype(F32)
    low = total - high - middle
    row = lax.broadcasted_iota(jnp.int32, (part, width), 0)
    tile = jnp.where(row == 0, high, jnp.where(row == 1, middle, jnp.where(row == 2, low, 0.0)))
    for z in range(nz):
        out_ref[z, size - part :] = tile.astype(BF16)


def pieces(at, v, basis, nz):
    mats, rows, rank = basis.shape
    part, width = rows // 8, 128
    return pl.pallas_call(
        pieces_kernel,
        out_shape=jax.ShapeDtypeStruct((nz, mats * part * rank // width + part, width), BF16),
        in_specs=[SMEM, VMEM, VMEM],
        out_specs=VMEM,
        compiler_params=PARAMS,
        cost_estimate=cost(2e9, 2**20),
        name="pieces",
    )(at, v, basis)


def pack_state_kernel(at_ref, one_ref, two_ref, *refs):
    outs, held_ref = refs[:-1], refs[-1]
    nz, _, cols = held_ref.shape
    ranks = one_ref.shape[1]
    for k, ref in enumerate((one_ref, two_ref)):
        for m in range(MATS):
            low = (k * MATS + m) * ranks
            for z in range(nz):
                held_ref[z, low : low + ranks] = ref[m, :, z * cols : (z + 1) * cols]
    for d in range(nz):
        outs[d][...] = held_ref[lax.rem(at_ref[3] + d, nz)]


def pack_state(at, one, two, nz):
    mats, ranks, cols = one.shape
    size = (2 * mats * ranks, cols // nz)
    return pl.pallas_call(
        pack_state_kernel,
        out_shape=[jax.ShapeDtypeStruct(size, F32)] * nz,
        in_specs=[SMEM, VMEM, VMEM],
        out_specs=[VMEM] * nz,
        scratch_shapes=[pltpu.VMEM((nz, *size), F32)],
        compiler_params=PARAMS,
        cost_estimate=cost(2e9, 2**20),
        name="pack_state",
    )(at, one, two)


def unpack_state_kernel(in_ref, one_ref, two_ref):
    nz, _, _ = in_ref.shape
    ranks = one_ref.shape[1]
    for k, ref in enumerate((one_ref, two_ref)):
        for m in range(MATS):
            low = (k * MATS + m) * ranks
            ref[m] = jnp.concatenate([in_ref[z, low : low + ranks] for z in range(nz)], axis=1)


def unpack_state(held):
    nz, kinds, cols = held.shape
    shape = jax.ShapeDtypeStruct((MATS, kinds // (2 * MATS), nz * cols), F32)
    return pl.pallas_call(
        unpack_state_kernel,
        out_shape=[shape, shape],
        in_specs=[VMEM],
        out_specs=[VMEM] * 2,
        compiler_params=PARAMS,
        cost_estimate=cost(2e9, 2**20),
        name="unpack_state",
    )(held)


def project_kernel(at_ref, g_ref, own_ref, peer_ref, basis_ref, *refs):
    outs, total_ref = refs[:-1], refs[-1]
    x, core, y = (at_ref[i] for i in range(3))
    nx, nz, size, width = own_ref.shape
    rank = basis_ref.shape[3]
    part = basis_ref.shape[2] // (2 * nx)
    count = rank // width
    cols = g_ref.shape[2]
    ny = len(outs)

    def gather(z, _):
        for m in range(MATS):
            for xa in range(nx):
                d = lax.rem(x - xa + nx, nx)
                for k in range(count):
                    low = (m * count + k) * part
                    ours, theirs = own_ref[d, z, low : low + part], peer_ref[d, z, low : low + part]
                    at = 2 * xa * part
                    lanes = slice(k * width, (k + 1) * width)
                    basis_ref[m, z, at : at + part, lanes] = jnp.where(core == 0, ours, theirs)
                    basis_ref[m, z, at + part : at + 2 * part, lanes] = jnp.where(
                        core == 0, theirs, ours
                    )
        return 0

    lax.fori_loop(0, nz, gather, 0)

    def multiply(m, _):
        left = jnp.concatenate([g_ref[z, m] for z in range(nz)], axis=1)
        right = basis_ref[m].reshape(left.shape[1], -1)
        total_ref[m] = jnp.dot(left, right, preferred_element_type=F32)
        return 0

    lax.fori_loop(0, MATS, multiply, 0)
    squares = jnp.zeros((part, width), F32)
    for ref in (own_ref, peer_ref):
        for d in range(nx):
            for z in range(nz):
                squares = squares + ref[d, z, size - part :].astype(F32)
    squares = jnp.sum(squares, axis=0, keepdims=True)
    for d in range(ny):
        start = pl.multiple_of(lax.rem(y + d, ny) * width, width)
        outs[d][:, :cols] = total_ref[:, :, pl.ds(start, width)]
        for m in range(MATS):
            outs[d][m, cols:] = jnp.broadcast_to(squares, (8, width))


def project(at, g, own, peer, rank, parts):
    nz, mats, cols, rows = g.shape
    basis, *out = pl.pallas_call(
        project_kernel,
        out_shape=[jax.ShapeDtypeStruct((mats, nz, rows, rank), BF16)]
        + [jax.ShapeDtypeStruct((mats, cols + 8, rank // parts), F32)] * parts,
        in_specs=[SMEM] + [VMEM] * 3,
        out_specs=[VMEM] * (1 + parts),
        scratch_shapes=[pltpu.VMEM((mats, cols, rank), F32)],
        compiler_params=PARAMS,
        cost_estimate=cost(2 * mats * nz * cols * rows * rank, 4 * 2**20),
        name="project",
    )(at, g, own, peer)
    return basis, out


def moments_kernel(at_ref, sum_ref, *refs):
    held, new_ref, update_ref, held_ref = refs[:-3], refs[-3], refs[-2], refs[-1]
    nz, kinds, cols = held_ref.shape
    ranks = kinds // (2 * MATS)
    for d in range(nz):
        held_ref[lax.rem(at_ref[3] - d + nz, nz)] = held[d][...]
    limit = 1.0 * math.sqrt(MATS * D * FF)
    scale = limit / jnp.maximum(jnp.sqrt(sum_ref[0, cols : cols + 1, 0:1]), limit)
    first_bias_correction = 1.0 - 0.9**STEP
    second_fix = 1.0 - 0.999**STEP
    spare = 256 - cols
    for m in range(MATS):
        one, two = (slice(k * ranks, (k + 1) * ranks) for k in (m, MATS + m))
        summed = sum_ref[m, :cols]
        padded = jnp.concatenate([summed, jnp.zeros((spare, summed.shape[1]), F32)], axis=0)
        scaled = scale * jnp.transpose(padded)[:, :cols]
        first = 0.9 * held_ref[:, one].reshape(nz * ranks, cols) + 0.1 * scaled
        second = 0.999 * held_ref[:, two].reshape(nz * ranks, cols) + 0.001 * scaled * scaled
        new_ref[:, one] = first.reshape(nz, ranks, cols)
        new_ref[:, two] = second.reshape(nz, ranks, cols)
        update = first / first_bias_correction / (jnp.sqrt(second / second_fix) + 1e-08)
        wide = jnp.concatenate([update, jnp.zeros((update.shape[0], spare), F32)], axis=1)
        update_ref[m] = jnp.transpose(wide)[:cols].astype(BF16)


def moments(at, summed, held):
    nz = len(held)
    kinds, cols = held[0].shape
    ranks = kinds // (2 * MATS)
    return pl.pallas_call(
        moments_kernel,
        out_shape=[
            jax.ShapeDtypeStruct((nz, kinds, cols), F32),
            jax.ShapeDtypeStruct((MATS, cols, nz * ranks), BF16),
        ],
        in_specs=[SMEM] + [VMEM] * (1 + nz),
        out_specs=[VMEM] * 2,
        scratch_shapes=[pltpu.VMEM((nz, kinds, cols), F32)],
        compiler_params=PARAMS,
        cost_estimate=cost(2e9, 2 * 2**20),
        name="moments",
    )(at, summed, *held)


def back_kernel(m, at_ref, basis_ref, w_ref, u0, u1, u2, u3, *refs):
    outs, whole_ref = refs[:-1], refs[-1]
    y, here = at_ref[2], at_ref[3]
    nz = basis_ref.shape[1]
    width = u0.shape[2]
    blocks = (u0, u1, u2, u3)
    n = len(blocks)
    for d in range(n):
        start = pl.multiple_of(lax.rem(y - d + n, n) * width, width)
        whole_ref[:, pl.ds(start, width)] = blocks[d][m]

    def rows(z):
        product = lax.dot_general(
            whole_ref[...], basis_ref[m, z], (((1,), (1,)), ((), ())), preferred_element_type=F32
        )
        return (w_ref[z, m].astype(F32) - 0.5 * product).astype(BF16)

    if len(outs) == 1:

        def store(z, _):
            outs[0][z] = rows(z)
            return 0

        lax.fori_loop(0, nz, store, 0)
    else:
        for d in range(nz):
            outs[d][...] = rows(lax.rem(here + d, nz))


def back(m, at, basis, w, blocks, apart):
    nz, _, cols, rows = w.shape
    rank = basis.shape[3]
    shapes = [(cols, rows)] * nz if apart else [(nz, cols, rows)]
    return pl.pallas_call(
        functools.partial(back_kernel, m),
        out_shape=[jax.ShapeDtypeStruct(shape, BF16) for shape in shapes],
        in_specs=[SMEM] + [VMEM] * 6,
        out_specs=[VMEM] * len(shapes),
        scratch_shapes=[pltpu.VMEM((cols, rank), BF16)],
        compiler_params=PARAMS,
        cost_estimate=cost(2 * nz * rows * cols * rank, 3 * 2**20),
        name="back",
    )(at, basis, w, *blocks)


def turn_kernel(at_ref, *refs):
    blocks, out_ref, held_ref = refs[:-2], refs[-2], refs[-1]
    nz, cols, rows = held_ref.shape
    for d in range(nz):
        held_ref[lax.rem(at_ref[3] - d + nz, nz)] = blocks[d][...]
    out_ref[...] = jnp.transpose(held_ref[...].reshape(nz * cols, rows))


def turn(at, blocks):
    nz = len(blocks)
    cols, rows = blocks[0].shape
    return pl.pallas_call(
        turn_kernel,
        out_shape=jax.ShapeDtypeStruct((rows, nz * cols), BF16),
        in_specs=[SMEM] + [VMEM] * nz,
        out_specs=VMEM,
        scratch_shapes=[pltpu.VMEM((nz, cols, rows), BF16)],
        compiler_params=PARAMS,
        cost_estimate=cost(2e9, 2**20),
        name="turn",
    )(at, *blocks)


def place_kernel(spots, at_ref, *refs):
    n = len(spots)
    blocks, out_ref, sems = refs[:n], refs[-2], refs[-1]
    x, core = at_ref[0], at_ref[1]
    copies = []
    for i, (m, dx, across, row) in enumerate(spots):
        rows, width = blocks[i].shape
        owner = lax.rem(x + dx, 4) * 2 + (1 - core if across else core)
        start = pl.multiple_of(owner * width, 128)
        copies.append(
            pltpu.make_async_copy(
                blocks[i], out_ref.at[m, pl.ds(row, rows), pl.ds(start, width)], sems.at[i]
            )
        )
    for copy in copies:
        copy.start()
    for copy in copies:
        copy.wait()


def place(whole, shape, at, items):
    spots = [item[1:] for item in items]
    blocks = [item[0] for item in items]
    n = len(blocks)
    given = () if whole is None else (whole,)
    size = sum(2 * 2 * b.size for b in blocks)
    return pl.pallas_call(
        functools.partial(place_kernel, spots),
        out_shape=jax.ShapeDtypeStruct(shape, BF16),
        in_specs=[SMEM] + [VMEM] * n + [ANY] * len(given),
        out_specs=ANY,
        scratch_shapes=[pltpu.SemaphoreType.DMA((n,))],
        input_output_aliases={} if whole is None else {n + 1: 0},
        compiler_params=PARAMS,
        cost_estimate=cost(2e9, size),
        name="place",
    )(at, *blocks, *given)


def step(grads, basis, moment1, moment2, weights):
    x, core = lax.axis_index("x"), lax.axis_index("core")
    y, z = lax.axis_index("y"), lax.axis_index("z")
    nx, nc, ny, nz = (lax.axis_size(a) for a in ("x", "core", "y", "z"))
    mats, rows, cols = grads.shape
    rank = basis.shape[2]
    at = jnp.stack([x, core, y, z])

    held = exchange(pieces(at, grads, basis, nz), "z")
    sent = pack(grads, nz)
    mine = exchange(sent, "z")
    w = pack(weights, nz)
    state = pack_state(at, moment1, moment2, nz)
    own = jnp.stack([held] + [shift(held, "x", k) for k in range(1, nx)])
    peer = shift(own, "core", 1)
    state = [state[0]] + [shift(state[k], "z", k) for k in range(1, nz)]
    w = exchange(before(mine, w), "z")

    gathered, parts = project(at, mine, own, peer, rank, ny)
    parts = [parts[0]] + [shift(parts[k], "y", k) for k in range(1, ny)]
    summed = (parts[0] + parts[1]) + (parts[2] + parts[3])
    news, update = moments(at, summed, state)
    updates = [update] + [shift(update, "y", k) for k in range(1, ny)]
    whole_block = back(0, at, gathered, w, updates, False)[0]
    whole_block = exchange(whole_block, "z")
    blocks = back(1, at, gathered, w, updates, True)
    moved = [blocks[0]]
    for k in range(1, nz):
        moved.append(shift(blocks[k], "z", k))
    turned = turn(at, moved)
    fresh = [jnp.swapaxes(whole_block.reshape(cols, rows), 0, 1), turned]
    news = exchange(before(whole_block, news), "z")
    news = unpack_state(news)

    half = rows // 2
    shape = (mats, rows, cols * nx * nc)

    def both(m, items):
        there = [(shift(b, "core", 1), m, dx, True, row) for b, dx, row in items]
        return [(b, m, dx, False, row) for b, dx, row in items] + there

    def put(whole, items):
        return place(whole, shape, at, items)

    near = []
    for f in fresh:
        left = shift(f, "x", 1)
        right = shift(f, "x", -1)
        near.append((left, right))

    def far(left, right):
        return shift(left[:half], "x", 1), shift(right[half:], "x", -1)

    def close(m):
        items = [(fresh[m], 0, 0), (near[m][0], 3, 0), (near[m][1], 1, 0)]
        return both(m, items)

    def distant(m, top, low):
        return both(m, [(top, 2, 0), (low, 2, half)])

    first = far(*near[0])
    whole = put(None, close(0))
    second = far(*near[1])
    whole = put(whole, distant(0, *first) + close(1))
    whole, *second = lax.optimization_barrier((whole, *second))
    whole = put(whole, distant(1, *second))
    return (whole, news[0], news[1])


def solution(mesh):
    finer = Mesh(mesh.devices.reshape(4, 2, 4, 8), ("x", "core", "y", "z"))
    dp, rows = ("x", "core"), ("y", "z")
    in_specs = (
        P(None, rows, dp),
        P(None, rows, None),
        P(None, rows, dp),
        P(None, rows, dp),
        P(None, rows, dp),
    )
    out_specs = (P(None, rows, None), P(None, rows, dp), P(None, rows, dp))
    return jax.shard_map(step, mesh=finer, in_specs=in_specs, out_specs=out_specs, check_vma=False)
```
